512 devices in a mesh: gx: 16 (over y, core), gz: 16 (over x, z_lo), grp: 2 (over z_hi).
Axes of the slice: x: 4, y: 8, z: 8 (z_hi: 2, z_lo: 4; z = z_hi * 4 + z_lo), core: 2. Of those that a mesh axis runs over, the one named last changes fastest.
Arguments:
- velocity: float32 [3, 3, 512, 2048], P(None, None, ('gz', 'grp'), 'gx'), may hold values from -5 to 5
- slab_average_downflow_speed: float32 [3], replicated, may hold values from 0.5 to 2
- mean_shear: float32 [3], replicated, may hold values from -2 to 2
- mode_counts: int32 [3, 2], replicated, may hold values from 64 to 128
Outputs:
- advanced: float32 [3, 3, 512, 2048], P(None, None, ('gz', 'grp'), 'gx')
- stress: float32 [6, 3, 512, 2048], P(None, None, ('gz', 'grp'), 'gx')
The draws below stay inside these ranges and needn't reach their ends.
All inputs are finite; a program needn't handle non-finite values.
Results may differ from the reference program's by a relative error of at most 0.00015.
Values sent between devices are 32-bit elements; how exact they have to be, the bound alone decides.
No kernel may reach another device: no remote copies, remote signals or barrier semaphores. Data moves between devices by JAX's collectives and lax.ppermute only.
A program may use at most 64 MiB of HBM per device.

```python
import math
import jax
import jax.numpy as jnp
from jax import lax

NX = 2048
NZ = 512
MODES = 256
PLANES = 3


def band_table(length, half_modes):
    positions = jnp.arange(length, dtype=jnp.int32)
    numbers = jnp.arange(half_modes, dtype=jnp.int32) + 1
    phase_int = positions[:, None] * numbers[None, :] % length
    angles = phase_int.astype(jnp.float32) * jnp.float32(2.0 * math.pi / length)
    return jnp.concatenate([jnp.cos(angles), jnp.sin(angles)], axis=1)


def draw_velocity(key, part):
    first_key, second_key = jax.random.split(jax.random.fold_in(key, 7101))
    half_modes = MODES // 2
    amplitude = jax.random.normal(first_key, (3, PLANES, 2 * half_modes, 2 * half_modes), jnp.float32) / half_modes
    table_x = band_table(NX, half_modes)
    table_z = band_table(NZ, half_modes)
    partial_sum = jnp.einsum('cpnm,xm->cpnx', amplitude, table_x, precision=lax.Precision.HIGHEST)
    banded = jnp.einsum('zn,cpnx->cpzx', table_z, partial_sum, precision=lax.Precision.HIGHEST)
    rough_part = 0.5 * jax.random.normal(second_key, (3, PLANES, NZ, NX), jnp.float32)
    return jnp.clip(banded + rough_part, -5.0, 5.0)


def place_ends(drawn, own_key, smallest, top_value):
    place = [jax.random.randint(jax.random.fold_in(own_key, axis), (), 0, length) for axis, length in enumerate(drawn.shape)]
    main_axis = drawn.shape.index(max(drawn.shape))
    next_to = place[:main_axis] + [(place[main_axis] + 1) % drawn.shape[main_axis]] + place[main_axis + 1:]
    return drawn.at[tuple(place)].set(smallest).at[tuple(next_to)].set(top_value)


def setup_inputs(seed: int = 0) -> dict:
    splits = jax.random.split(jax.random.key(seed), 5)
    return {
        "velocity": draw_velocity(jax.random.fold_in(splits[4], 71), 0),
        "slab_average_downflow_speed": jnp.clip(jax.random.uniform(splits[1], (PLANES,), jnp.float32, 0.5, 2.0), 0.5, 2.0),
        "mean_shear": jnp.clip(jax.random.uniform(splits[2], (PLANES,), jnp.float32, -2.0, 2.0), -2.0, 2.0),
        "mode_counts": place_ends(jax.random.randint(splits[3], (PLANES, 2), MODES // 4, MODES // 2 + 1), jax.random.fold_in(splits[3], 1), MODES // 4, (MODES // 2 + 1) - 1).astype(jnp.int32),
    }


molecular_diffusivity = 0.4
time_step = 0.2
highest = lax.Precision.HIGHEST


def wave_numbers(modes):
    column = jnp.arange(modes, dtype=jnp.int32)
    half_modes = modes // 2
    return jnp.where(column < half_modes, column, column - half_modes + 1)


def wave_table(positions, length, modes):
    column = jnp.arange(modes, dtype=jnp.int32)
    numbers = wave_numbers(modes)
    phase_int = (positions[:, None] * numbers[None, :]) % length
    angles = phase_int.astype(jnp.float32) * jnp.float32(2.0 * math.pi / length)
    return jnp.where(column[None, :] < modes // 2, jnp.cos(angles), jnp.sin(angles))


def mode_weights(length, modes):
    column = jnp.arange(modes, dtype=jnp.int32)
    return jnp.where(column == 0, jnp.float32(1.0 / length), jnp.float32(2.0 / length))


def tendency_from(middle_entry, east_cells, west_cells, north_cells, south_cells, slab_average_downflow_speed, mean_shear):
    downflow_derivative_field = (east_cells - west_cells) * 0.5
    crossflow_derivative_field = (north_cells - south_cells) * 0.5
    diffusion_contribution = east_cells + west_cells + north_cells + south_cells - 4.0 * middle_entry
    holding_slab = slab_average_downflow_speed[:, None, None] + middle_entry[0]
    advanced_state = -holding_slab[None] * downflow_derivative_field - middle_entry[2][None] * crossflow_derivative_field + molecular_diffusivity * diffusion_contribution
    shear_term = mean_shear[:, None, None] * middle_entry[1]
    return jnp.concatenate([advanced_state[0:1] - shear_term[None], advanced_state[1:]], axis=0)


def runge_kutta(velocity, rate):
    first = velocity + time_step * rate(velocity)
    second = 0.75 * velocity + 0.25 * (first + time_step * rate(first))
    return velocity / 3.0 + (2.0 / 3.0) * (second + time_step * rate(second))


def reference(velocity, slab_average_downflow_speed, mean_shear, mode_counts):
    def rate(field):
        return tendency_from(field, jnp.roll(field, -1, axis=3), jnp.roll(field, 1, axis=3),
                             jnp.roll(field, -1, axis=2), jnp.roll(field, 1, axis=2), slab_average_downflow_speed, mean_shear)

    advanced = runge_kutta(velocity, rate)
    table_x = wave_table(jnp.arange(NX, dtype=jnp.int32), NX, MODES)
    table_z = wave_table(jnp.arange(NZ, dtype=jnp.int32), NZ, MODES)
    analysis_x = table_x * mode_weights(NX, MODES)[None, :]
    analysis_z = table_z * mode_weights(NZ, MODES)[None, :]
    numbers = wave_numbers(MODES)
    keep_z = numbers[None, :] <= mode_counts[:, 1][:, None]
    keep_x = numbers[None, :] <= mode_counts[:, 0][:, None]
    keep = (keep_z[:, :, None] & keep_x[:, None, :]).astype(jnp.float32)

    def filter_field(field):
        coeffs = jnp.einsum('pzx,xm->pzm', field, analysis_x, precision=highest)
        coeffs = jnp.einsum('pzm,zn->pnm', coeffs, analysis_z, precision=highest) * keep
        partial_sum = jnp.einsum('pnm,zn->pzm', coeffs, table_z, precision=highest)
        return jnp.einsum('pzm,xm->pzx', partial_sum, table_x, precision=highest)

    filtered_velocity = lax.map(filter_field, advanced)
    pair_first = jnp.array([0, 0, 0, 1, 1, 2], dtype=jnp.int32)
    pair_second = jnp.array([0, 1, 2, 1, 2, 2], dtype=jnp.int32)

    def one_stress(index):
        first_idx = pair_first[index]
        second_idx = pair_second[index]
        product = advanced[first_idx] * advanced[second_idx]
        return filter_field(product) - filtered_velocity[first_idx] * filtered_velocity[second_idx]

    stress = lax.map(one_stress, jnp.arange(6, dtype=jnp.int32))
    return advanced, stress
```

```python
import math

import jax
import jax.numpy as jnp
import numpy as np
from jax import lax
from jax.experimental import pallas as pl
from jax.experimental.pallas import tpu as pltpu
from jax.sharding import PartitionSpec as P

NX = 2048
NZ = 512
MODES = 256
HALF = MODES // 2
PLANES = 3
TILE_Z = 16
TILE_X = 128
GX = NX // TILE_X
GZ = NZ // TILE_Z
LANES = 128

molecular_diffusivity = 0.4
time_step = 0.2
highest = lax.Precision.HIGHEST
spanwise = ("gz", "grp")
pair_first = (0, 0, 0, 1, 1, 2)
pair_second = (0, 1, 2, 1, 2, 2)


def roll(values, shift, axis):
    return pltpu.roll(values, shift % values.shape[axis], axis)


def call(body, out_shapes, smem, *args):
    count = len(args)

    def kernel(*refs):
        ins = list(refs[:smem]) + [ref[...] for ref in refs[smem:count]]
        for ref, value in zip(refs[count:], body(*ins)):
            ref[...] = value

    return pl.pallas_call(
        kernel,
        out_shape=[jax.ShapeDtypeStruct(shape, jnp.float32) for shape in out_shapes],
        in_specs=[pl.BlockSpec(memory_space=pltpu.SMEM)] * smem
        + [pl.BlockSpec(memory_space=pltpu.VMEM)] * (count - smem),
        out_specs=[pl.BlockSpec(memory_space=pltpu.VMEM)] * len(out_shapes),
    )(*args)


def dot(left, right, left_dim=1, right_dim=0):
    return lax.dot_general(
        left,
        right,
        (((left_dim,), (right_dim,)), ((), ())),
        precision=highest,
        preferred_element_type=jnp.float32,
    )


def rate(components, downflow, shear):
    rates = []
    for index, cells in enumerate(components):
        east = roll(cells, -1, 1)
        west = roll(cells, 1, 1)
        north = roll(cells, -1, 0)
        south = roll(cells, 1, 0)
        result = (
            -(downflow + components[0]) * ((east - west) * 0.5)
            - components[2] * ((north - south) * 0.5)
            + molecular_diffusivity * (east + west + north + south - 4.0 * cells)
        )
        if index == 0:
            result = result - shear * components[1]
        rates.append(result)
    return rates


def advance_body(downflow, shear, own, left, right, synth_x):
    lane = lax.broadcasted_iota(jnp.int32, (24, LANES), 1)
    stepped = [[None] * PLANES for _ in range(3)]
    for p in range(PLANES):
        start = [
            jnp.concatenate(
                [own[c, p], jnp.where(lane < LANES // 2, right[c, p], left[c, p])], axis=1
            )
            for c in range(3)
        ]
        slope = rate(start, downflow[p], shear[p])
        first = [v + time_step * r for v, r in zip(start, slope)]
        slope = rate(first, downflow[p], shear[p])
        second = [
            0.75 * v + 0.25 * (f + time_step * r) for v, f, r in zip(start, first, slope)
        ]
        slope = rate(second, downflow[p], shear[p])
        for c in range(3):
            last = start[c] * (1.0 / 3.0) + (2.0 / 3.0) * (second[c] + time_step * slope[c])
            stepped[c][p] = last[:TILE_Z, :TILE_X]
    fields = [stepped[c][p] for c in range(3) for p in range(PLANES)]
    for a, b in zip(pair_first, pair_second):
        fields += [stepped[a][p] * stepped[b][p] for p in range(PLANES)]
    sums = []
    for tile in range(3):
        rows = jnp.concatenate(fields[8 * tile : 8 * tile + 8], axis=0)
        sums.append(dot(synth_x, rows, 1, 1).reshape(GX, 16, LANES))
    blank = jnp.zeros((TILE_Z, TILE_X), jnp.float32)
    rows = jnp.concatenate((fields[24:] + [blank]) * 2, axis=0)
    rest = dot(synth_x, rows, 1, 1).reshape(GX, 2, 8, LANES)
    lane = lax.broadcasted_iota(jnp.int32, (GX, 8, LANES), 2)
    sums.append(jnp.where(lane < LANES // 2, rest[:, 0], rest[:, 1]))
    advanced = jnp.stack([jnp.stack(stepped[c]) for c in range(3)])
    return advanced, jnp.concatenate(sums, axis=1)


def total_body(tiles):
    total = tiles[0]
    for index in range(1, GX):
        total = total + tiles[index]
    rest = total[48:56]
    lane = lax.broadcasted_iota(jnp.int32, (16, LANES), 1)
    rest = jnp.concatenate([rest, roll(rest, LANES // 2, 1)], axis=0)
    rest = jnp.where(lane < LANES // 2, rest, 0.0)
    upper = jnp.concatenate([total[0:16], total[16:32]], axis=1)
    lower = jnp.concatenate([total[32:48], rest], axis=1)
    return (jnp.concatenate([upper, lower], axis=0),)


def spanwise_body(place, counts, lines, analysis_z, synth_z):
    width = 2 * LANES
    in_block = lax.broadcasted_iota(jnp.int32, (GZ, width), 1) % TILE_Z
    spread = jnp.concatenate(
        [jnp.where(in_block == row, lines, 0.0) for row in range(TILE_Z)], axis=0
    )
    partial_sum = dot(analysis_z, spread)
    group = lax.broadcasted_iota(jnp.int32, (width, width), 0) // TILE_Z
    other = lax.broadcasted_iota(jnp.int32, (width, width), 1) // TILE_Z
    coeffs = dot(partial_sum, jnp.where(group == other, 1.0, 0.0))
    mode_x = place[0]
    number_x = jnp.where(mode_x < HALF, mode_x, mode_x - HALF + 1)
    weight_x = jnp.where(mode_x == 0, 1.0 / NX, 2.0 / NX)
    mode_z = lax.broadcasted_iota(jnp.int32, (MODES, width), 0)
    number_z = jnp.where(mode_z < HALF, mode_z, mode_z - HALF + 1)
    lane = lax.broadcasted_iota(jnp.int32, (MODES, width), 1)
    plane = (lane // TILE_Z + place[1]) % PLANES
    limit = jnp.zeros((MODES, width), jnp.int32)
    for p in range(PLANES):
        kept = jnp.where(number_x <= counts[p, 0], counts[p, 1], -1)
        limit = jnp.where(plane == p, kept, limit)
    coeffs = jnp.where(number_z <= limit, coeffs * weight_x, 0.0)
    rows = dot(synth_z, coeffs)
    result = jnp.zeros((GZ, width), jnp.float32)
    for row in range(TILE_Z):
        result = jnp.where(in_block == row, rows[row * GZ : (row + 1) * GZ], result)
    return (result,)


def stress_body(coeffs, synth_x):
    halves = []
    for half in range(2):
        block = coeffs[:, 16 * half : 16 * half + 16].reshape(MODES, 2 * LANES)
        halves.append(dot(block, synth_x, 0, 0))

    def filtered(field, plane):
        index = field * PLANES + plane
        start = index % 16 * TILE_Z
        return halves[index // 16][start : start + TILE_Z]

    stresses = []
    for q, (a, b) in enumerate(zip(pair_first, pair_second)):
        stresses.append(
            jnp.stack(
                [
                    filtered(3 + q, p) - filtered(a, p) * filtered(b, p)
                    for p in range(PLANES)
                ]
            )
        )
    return (jnp.stack(stresses),)


def spanwise_tables():
    column = np.arange(MODES)
    numbers = np.where(column < HALF, column, column - HALF + 1)
    positions = (np.arange(GZ)[None, :] * TILE_Z + np.arange(TILE_Z)[:, None]).reshape(-1)
    angles = (positions[:, None] * numbers[None, :] % NZ) * (2.0 * math.pi / NZ)
    synth = np.where(column[None, :] < HALF, np.cos(angles), np.sin(angles))
    weights = np.where(column == 0, 1.0 / NZ, 2.0 / NZ)
    analysis = (synth * weights[None, :]).T
    return np.ascontiguousarray(analysis, np.float32), synth.astype(np.float32)


def streamwise_table(start):
    column = jnp.arange(MODES, dtype=jnp.int32)
    numbers = jnp.where(column < HALF, column, column - HALF + 1)
    positions = start + jnp.arange(TILE_X, dtype=jnp.int32)
    phase_int = numbers[:, None] * positions[None, :] % NX
    angles = phase_int.astype(jnp.float32) * jnp.float32(2.0 * math.pi / NX)
    return jnp.where(column[:, None] < HALF, jnp.cos(angles), jnp.sin(angles))


def neighbours(lower, upper, axis):
    count = lax.axis_size(axis)
    before = lax.ppermute(upper, axis, [(i, (i + 1) % count) for i in range(count)])
    after = lax.ppermute(lower, axis, [((i + 1) % count, i) for i in range(count)])
    return before, after


def local(velocity, downflow, shear, mode_counts):
    here_x = lax.axis_index("gx")
    here_z = lax.axis_index(spanwise)
    above, below = neighbours(velocity[:, :, :3], velocity[:, :, -3:], spanwise)
    gap = jnp.zeros((3, PLANES, 2, TILE_X), jnp.float32)
    own = jnp.concatenate([velocity, below, gap, above], axis=2)
    left, right = neighbours(own, own, "gx")
    synth_x = streamwise_table(here_x * TILE_X)
    analysis_z, synth_z = (jnp.asarray(table) for table in spanwise_tables())

    advanced, sums = call(
        advance_body,
        [(3, PLANES, TILE_Z, TILE_X), (GX, 56, LANES)],
        2,
        downflow,
        shear,
        own,
        left,
        right,
        synth_x,
    )
    sums = lax.all_to_all(sums, "gx", 0, 0, tiled=True)
    (lines,) = call(total_body, [(GZ, 2 * LANES)], 0, sums)
    lines = lax.all_to_all(lines, spanwise, 0, 0, tiled=True)
    place = jnp.stack([here_x * 16 + here_z % 16, here_z // 16 * 16])
    (lines,) = call(
        spanwise_body,
        [(GZ, 2 * LANES)],
        2,
        place,
        mode_counts,
        lines,
        analysis_z,
        synth_z,
    )
    lines = lax.all_to_all(lines, spanwise, 0, 0, tiled=True)
    coeffs = lax.all_gather(lines, "gx")
    (stress,) = call(stress_body, [(6, PLANES, TILE_Z, TILE_X)], 0, coeffs, synth_x)
    return advanced, stress


def solution(mesh):
    return jax.shard_map(
        local,
        mesh=mesh,
        in_specs=(P(None, None, ("gz", "grp"), "gx"), P(), P(), P()),
        out_specs=(P(None, None, ("gz", "grp"), "gx"), P(None, None, ("gz", "grp"), "gx")),
        check_vma=False,
    )
```

```python
import math

import jax
import jax.numpy as jnp
import numpy as np
from jax import lax
from jax.experimental import pallas as pl
from jax.experimental.pallas import tpu as pltpu
from jax.sharding import PartitionSpec as P

NX = 2048
NZ = 512
MODES = 256
HALF = MODES // 2
PLANES = 3
TILE_Z = 16
TILE_X = 128
GX = NX // TILE_X
GZ = NZ // TILE_Z
LANES = 128

SLOT = 14
STRIDE = PLANES * SLOT

molecular_diffusivity = 0.4
time_step = 0.2
highest = lax.Precision.HIGHEST
spanwise = ("gz", "grp")
pair_first = (0, 0, 0, 1, 1, 2)
pair_second = (0, 1, 2, 1, 2, 2)


def roll(values, shift, axis):
    shift = shift % values.shape[axis]
    return pltpu.roll(values, shift, axis) if shift else values


def call(body, out_shapes, smem, scratch, *args):
    return pl.pallas_call(
        body,
        out_shape=[jax.ShapeDtypeStruct(shape, jnp.float32) for shape in out_shapes],
        in_specs=[pl.BlockSpec(memory_space=pltpu.SMEM)] * smem
        + [pl.BlockSpec(memory_space=pltpu.VMEM)] * (len(args) - smem),
        out_specs=[pl.BlockSpec(memory_space=pltpu.VMEM)] * len(out_shapes),
        scratch_shapes=[pltpu.VMEM(shape, jnp.float32) for shape in scratch],
    )(*args)


def dot(left, right):
    return lax.dot_general(
        left,
        right,
        (((1,), (0,)), ((), ())),
        precision=highest,
        preferred_element_type=jnp.float32,
    )


def lanes_of(rows):
    return lax.broadcasted_iota(jnp.int32, (rows, LANES), 1)


def pack_body(own, left, right, out):
    lane = lanes_of(TILE_Z)
    cells = [own[c, p] for c in range(3) for p in range(PLANES)]
    for dest in range(GZ):
        if dest == 0:
            sides = [
                jnp.where(lane < LANES // 2, own[c, p], left[c, p])
                for c in range(3)
                for p in range(PLANES)
            ]
        elif dest == GZ - 1:
            sides = [
                jnp.where(lane < LANES // 2, right[c, p], own[c, p])
                for c in range(3)
                for p in range(PLANES)
            ]
        else:
            sides = cells
        packed = jnp.zeros((TILE_Z, LANES), jnp.float32)
        for index, values in enumerate(sides):
            moved = roll(values, index * SLOT - (4 * dest - 3), 1)
            here = (lane >= index * SLOT) & (lane < index * SLOT + 10)
            packed = jnp.where(here, moved, packed)
        out[dest] = packed


def advance_body(
    downflow, shear, counts, cells, table, sort_fields, sort_cells,
    out, start, first, second,
):
    chunk = 64
    edge = 8
    lane = lanes_of(chunk)
    component = lane // STRIDE
    plane = lane % STRIDE // SLOT
    flow = jnp.zeros((chunk, LANES), jnp.float32)
    slope = jnp.zeros((chunk, LANES), jnp.float32)
    for p in range(PLANES):
        flow = jnp.where(plane == p, downflow[p], flow)
        slope = jnp.where((plane == p) & (component == 0), shear[p], slope)

    def store(ref, row, values):
        ref[edge + row : edge + row + chunk] = values
        if row == 0:
            ref[edge + NZ : edge + NZ + edge] = values[:edge]
        if row == NZ - chunk:
            ref[:edge] = values[chunk - edge :]

    def rate(ref, row):
        low = edge + row
        middle = ref[low : low + chunk]
        north = ref[low + 1 : low + 1 + chunk]
        south = ref[low - 1 : low - 1 + chunk]
        east = roll(middle, -1, 1)
        west = roll(middle, 1, 1)
        next_one = roll(middle, -STRIDE, 1)
        along = jnp.where(
            component == 0,
            middle,
            jnp.where(component == 1, roll(middle, STRIDE, 1), roll(middle, 2 * STRIDE, 1)),
        )
        across = jnp.where(
            component == 2,
            middle,
            jnp.where(component == 1, next_one, roll(middle, -2 * STRIDE, 1)),
        )
        return middle, (
            -(flow + along) * ((east - west) * 0.5)
            - across * ((north - south) * 0.5)
            + molecular_diffusivity * (east + west + north + south - 4.0 * middle)
            - slope * next_one
        )

    rows = range(0, NZ, chunk)
    for row in rows:
        store(start, row, cells[row // 16 : (row + chunk) // 16].reshape(chunk, LANES))
    for row in rows:
        middle, change = rate(start, row)
        store(first, row, middle + time_step * change)
    for row in rows:
        middle, change = rate(first, row)
        begin = start[edge + row : edge + row + chunk]
        store(second, row, 0.75 * begin + 0.25 * (middle + time_step * change))
    part = (lane + LANES - 3) % LANES % SLOT // 4
    part = jnp.where((lane >= 3) & (lane < 127), part, 3)
    for row in rows:
        middle, change = rate(second, row)
        begin = start[edge + row : edge + row + chunk]
        last = begin * (1.0 / 3.0) + (2.0 / 3.0) * (middle + time_step * change)
        other = jnp.where(component == 2, roll(last, 2 * STRIDE, 1), roll(last, -STRIDE, 1))
        fields = jnp.where(part == 0, last, 0.0)
        fields = jnp.where(part == 1, roll(last * last, 4, 1), fields)
        first[row : row + chunk] = jnp.where(part == 2, roll(last * other, 8, 1), fields)
        sorted_cells = dot(jnp.where(part == 0, last, 0.0), sort_cells[...])
        sorted_cells = sorted_cells.reshape(chunk // 16, 2, 8, LANES)
        side = lax.broadcasted_iota(jnp.int32, (chunk // 16, 8, LANES), 2)
        out[row // 16 : (row + chunk) // 16, 16:24] = jnp.where(
            side < LANES // 2, sorted_cells[:, 0], sorted_cells[:, 1]
        )
    coeffs = dot(dot(table[...], first[:NZ]), sort_fields[...])
    mode = lax.broadcasted_iota(jnp.int32, (MODES, LANES), 0)
    number = jnp.where(mode < HALF, mode, mode - HALF + 1)
    plane = lanes_of(MODES) % 32 % PLANES
    limit = jnp.zeros((MODES, LANES), jnp.int32)
    for p in range(PLANES):
        limit = jnp.where(plane == p, counts[p, 1], limit)
    weight = jnp.where(mode == 0, 1.0 / NZ, 2.0 / NZ)
    coeffs = jnp.where(number <= limit, coeffs * weight, 0.0)
    out[:, 0:16] = dot(table[...].T, coeffs).reshape(GZ, 16, LANES)


def forward_body(cells, out):
    for row in range(TILE_Z):
        out[row] = cells[:, row, :]


def unsort():
    source = lax.broadcasted_iota(jnp.int32, (LANES, LANES), 0)
    target = lax.broadcasted_iota(jnp.int32, (LANES, LANES), 1)
    return jnp.where(target == source % 32 * 4 + source // 32, 1.0, 0.0)


def cells_body(cells, out, rows):
    lane = lanes_of(16)
    order = unsort()
    for group in range(2):
        stacked = jnp.concatenate(
            [cells[:, 16 + 4 * group + r, :] for r in range(4)], axis=0
        )
        turned = stacked.T
        for half in range(2):
            for r in range(4):
                joined = jnp.zeros((16, LANES), jnp.float32)
                for column in range(4):
                    begin = half * 64 + column * 16
                    moved = roll(turned[begin : begin + 16], (column - r) * 32, 1)
                    joined = jnp.where(lane // 32 == column, moved, joined)
                place = (half * 8 + group * 4 + r) * 16
                rows[place : place + 16] = joined
    rows[...] = dot(rows[...], order)
    for c in range(3):
        for p in range(PLANES):
            out[c, p] = rows[pl.ds(c * PLANES + p, TILE_Z, stride=16), :]


def streamwise_body(counts, lines, table, out, rows):
    cells = lines[...].reshape(NX // 4, LANES)
    coeffs = dot(table[0], cells)
    for column in range(1, 4):
        coeffs = coeffs + roll(dot(table[column], cells), -32 * column, 1)
    mode = lax.broadcasted_iota(jnp.int32, (MODES, LANES), 0)
    number = jnp.where(mode < HALF, mode, mode - HALF + 1)
    weight = jnp.where(mode == 0, 1.0 / NX, 2.0 / NX)
    lane = lanes_of(MODES)
    limit = jnp.full((MODES, LANES), -1, jnp.int32)
    for p in range(PLANES):
        limit = jnp.where((lane < 27) & (lane % PLANES == p), counts[p, 0], limit)
    coeffs = jnp.where(number <= limit, coeffs * weight, 0.0).T[:32]
    rows[...] = jnp.zeros(rows.shape, jnp.float32)
    for column in range(4):
        filtered = dot(coeffs, table[column])
        for q, (a, b) in enumerate(zip(pair_first, pair_second)):
            rows[column, 3 * q : 3 * q + 3] = (
                filtered[9 + 3 * q : 12 + 3 * q]
                - filtered[3 * a : 3 * a + 3] * filtered[3 * b : 3 * b + 3]
            )
    lane = lanes_of(24)
    for dest in range(GX):
        begin = dest // 4 * LANES
        joined = jnp.zeros((24, LANES), jnp.float32)
        for column in range(4):
            moved = roll(rows[column, :, begin : begin + LANES], (column - dest % 4) * 32, 1)
            joined = jnp.where(lane // 32 == column, moved, joined)
        out[dest] = joined


def stress_body(lines, out, rows):
    rows[...] = dot(lines[...].reshape(16 * 24, LANES), unsort())
    for q in range(6):
        for p in range(PLANES):
            out[q, p] = rows[pl.ds(q * PLANES + p, TILE_Z, stride=24), :]


def wave_table(length):
    column = np.arange(MODES)
    numbers = np.where(column < HALF, column, column - HALF + 1)
    angles = (np.arange(length)[:, None] * numbers[None, :] % length) * (2.0 * math.pi / length)
    return np.where(column[None, :] < HALF, np.cos(angles), np.sin(angles))


def tables():
    synth_z = wave_table(NZ).T
    synth_x = wave_table(NX).reshape(NX // 4, 4, MODES).transpose(1, 2, 0)
    sort_fields = np.zeros((LANES, LANES))
    sort_cells = np.zeros((LANES, LANES))
    kinds = ((0, 1, 2), (3, 6, 8), (4, 7, 5))
    for c in range(3):
        for p in range(PLANES):
            for column in range(4):
                lane = c * STRIDE + p * SLOT + 3 + column
                for kind in range(3):
                    field = kinds[kind][c] * PLANES + p
                    sort_fields[lane + 4 * kind, column * 32 + field] = 1.0
                for half in range(2):
                    sort_cells[lane, half * 64 + column * 16 + c * PLANES + p] = 1.0
    return [
        jnp.asarray(np.ascontiguousarray(values, dtype=np.float32))
        for values in (synth_z, sort_fields, sort_cells, synth_x)
    ]


def local(velocity, downflow, shear, mode_counts):
    count = lax.axis_size("gx")
    left = lax.ppermute(velocity, "gx", [(i, (i + 1) % count) for i in range(count)])
    right = lax.ppermute(velocity, "gx", [((i + 1) % count, i) for i in range(count)])
    synth_z, sort_fields, sort_cells, synth_x = tables()
    (cells,) = call(pack_body, [(GZ, TILE_Z, LANES)], 0, [], velocity, left, right)
    cells = lax.all_to_all(cells, spanwise, 0, 0, tiled=True)
    (cells,) = call(
        advance_body,
        [(GZ, 24, LANES)],
        3,
        [(NZ + 16, LANES)] * 3,
        downflow,
        shear,
        mode_counts,
        cells,
        synth_z,
        sort_fields,
        sort_cells,
    )
    cells = lax.all_to_all(cells, spanwise, 0, 0, tiled=True)
    (lines,) = call(forward_body, [(GX, GZ, LANES)], 0, [], cells)
    lines = lax.all_to_all(lines, "gx", 0, 0, tiled=True)
    (advanced,) = call(
        cells_body, [(3, PLANES, TILE_Z, TILE_X)], 0, [(16 * TILE_Z, LANES)], cells
    )
    (lines,) = call(
        streamwise_body,
        [(GX, 24, LANES)],
        1,
        [(4, 24, NX // 4)],
        mode_counts,
        lines,
        synth_x,
    )
    lines = lax.all_to_all(lines, "gx", 0, 0, tiled=True)
    (stress,) = call(
        stress_body, [(6, PLANES, TILE_Z, TILE_X)], 0, [(16 * 24, LANES)], lines
    )
    return advanced, stress


def solution(mesh):
    return jax.shard_map(
        local,
        mesh=mesh,
        in_specs=(P(None, None, ("gz", "grp"), "gx"), P(), P(), P()),
        out_specs=(P(None, None, ("gz", "grp"), "gx"), P(None, None, ("gz", "grp"), "gx")),
        check_vma=False,
    )
```

```python
import math

import jax
import jax.numpy as jnp
import numpy as np
from jax import lax
from jax.experimental import pallas as pl
from jax.experimental.pallas import tpu as pltpu
from jax.sharding import PartitionSpec as P

NX = 2048
NZ = 512
MODES = 256
HALF = MODES // 2
PLANES = 3
TILE_Z = 16
TILE_X = 128
GX = NX // TILE_X
GZ = NZ // TILE_Z
LANES = 128

SLOT = 14
STRIDE = PLANES * SLOT

molecular_diffusivity = 0.4
time_step = 0.2
highest = lax.Precision.HIGHEST
spanwise = ("gz", "grp")
pair_first = (0, 0, 0, 1, 1, 2)
pair_second = (0, 1, 2, 1, 2, 2)


def roll(values, shift, axis):
    shift = shift % values.shape[axis]
    return pltpu.roll(values, shift, axis) if shift else values


def call(body, out_shapes, smem, scratch, *args, tables=0, final=False, alias=None):
    make = jax.ShapeDtypeStruct if final else pltpu.VMEM
    near = len(args) - tables
    args = (
        args[:smem]
        + tuple(pltpu.with_memory_space_constraint(arg, pltpu.VMEM) for arg in args[smem:near])
        + args[near:]
    )
    fetched = [pltpu.VMEM(arg.shape, arg.dtype) for arg in args[near:]]
    return pl.pallas_call(
        body,
        out_shape=[make(shape, jnp.float32) for shape in out_shapes],
        in_specs=[pl.BlockSpec(memory_space=pltpu.SMEM)] * smem
        + [pl.BlockSpec(memory_space=pltpu.VMEM)] * (near - smem)
        + [pl.BlockSpec(memory_space=pl.ANY)] * tables,
        out_specs=[pl.BlockSpec(memory_space=pltpu.VMEM)] * len(out_shapes),
        scratch_shapes=[pltpu.VMEM(shape, jnp.float32) for shape in scratch]
        + fetched
        + ([pltpu.SemaphoreType.DMA((4,))] if tables else []),
        input_output_aliases=alias or {},
    )(*args)


def dot(left, right):
    return lax.dot_general(
        left,
        right,
        (((1,), (0,)), ((), ())),
        precision=highest,
        preferred_element_type=jnp.float32,
    )


def lanes_of(rows):
    return lax.broadcasted_iota(jnp.int32, (rows, LANES), 1)


def packed_for(dest, sides):
    lane = lanes_of(TILE_Z)
    packed = jnp.zeros((TILE_Z, LANES), jnp.float32)
    for index, values in enumerate(sides):
        moved = roll(values, index * SLOT - (4 * dest - 3), 1)
        here = (lane >= index * SLOT) & (lane < index * SLOT + 10)
        packed = jnp.where(here, moved, packed)
    return packed


def inner_body(own, out):
    cells = [own[c, p] for c in range(3) for p in range(PLANES)]
    for dest in range(1, GZ - 1):
        out[dest] = packed_for(dest, cells)
    out[0] = packed_for(GZ // 2, cells)
    out[GZ - 1] = packed_for(GZ // 2, cells)


def outer_body(own, left, right, inner, out):
    low = lanes_of(TILE_Z) < LANES // 2
    pairs = [(c, p) for c in range(3) for p in range(PLANES)]
    out[0] = packed_for(0, [jnp.where(low, own[c, p], left[c, p]) for c, p in pairs])
    out[GZ - 1] = packed_for(
        GZ - 1, [jnp.where(low, right[c, p], own[c, p]) for c, p in pairs]
    )


def advance_body(
    downflow, shear, counts, cells, far_table, far_fields, far_cells,
    out, start, first, second, table, sort_fields, sort_cells, done,
):
    fetch_table = pltpu.make_async_copy(far_table, table, done.at[0])
    fetch_fields = pltpu.make_async_copy(far_fields, sort_fields, done.at[1])
    fetch_cells = pltpu.make_async_copy(far_cells, sort_cells, done.at[2])
    fetch_cells.start()
    fetch_table.start()
    fetch_fields.start()
    chunk = 64
    edge = 8
    lane = lanes_of(chunk)
    component = lane // STRIDE
    plane = lane % STRIDE // SLOT
    flow = jnp.zeros((chunk, LANES), jnp.float32)
    slope = jnp.zeros((chunk, LANES), jnp.float32)
    for p in range(PLANES):
        flow = jnp.where(plane == p, downflow[p], flow)
        slope = jnp.where((plane == p) & (component == 0), shear[p], slope)

    def store(ref, row, values):
        ref[edge + row : edge + row + chunk] = values
        if row == 0:
            ref[edge + NZ : edge + NZ + edge] = values[:edge]
        if row == NZ - chunk:
            ref[:edge] = values[chunk - edge :]

    def rate(ref, row):
        low = edge + row
        middle = ref[low : low + chunk]
        north = ref[low + 1 : low + 1 + chunk]
        south = ref[low - 1 : low - 1 + chunk]
        east = roll(middle, -1, 1)
        west = roll(middle, 1, 1)
        next_one = roll(middle, -STRIDE, 1)
        along = jnp.where(
            component == 0,
            middle,
            jnp.where(component == 1, roll(middle, STRIDE, 1), roll(middle, 2 * STRIDE, 1)),
        )
        across = jnp.where(
            component == 2,
            middle,
            jnp.where(component == 1, next_one, roll(middle, -2 * STRIDE, 1)),
        )
        return middle, (
            -(flow + along) * ((east - west) * 0.5)
            - across * ((north - south) * 0.5)
            + molecular_diffusivity * (east + west + north + south - 4.0 * middle)
            - slope * next_one
        )

    rows = range(0, NZ, chunk)
    for row in rows:
        store(start, row, cells[row // 16 : (row + chunk) // 16].reshape(chunk, LANES))
    for row in rows:
        middle, change = rate(start, row)
        store(first, row, middle + time_step * change)
    for row in rows:
        middle, change = rate(first, row)
        begin = start[edge + row : edge + row + chunk]
        store(second, row, 0.75 * begin + 0.25 * (middle + time_step * change))
    fetch_cells.wait()
    part = (lane + LANES - 3) % LANES % SLOT // 4
    part = jnp.where((lane >= 3) & (lane < 127), part, 3)
    for row in rows:
        middle, change = rate(second, row)
        begin = start[edge + row : edge + row + chunk]
        last = begin * (1.0 / 3.0) + (2.0 / 3.0) * (middle + time_step * change)
        other = jnp.where(component == 2, roll(last, 2 * STRIDE, 1), roll(last, -STRIDE, 1))
        fields = jnp.where(part == 0, last, 0.0)
        fields = jnp.where(part == 1, roll(last * last, 4, 1), fields)
        first[row : row + chunk] = jnp.where(part == 2, roll(last * other, 8, 1), fields)
        sorted_cells = dot(jnp.where(part == 0, last, 0.0), sort_cells[...])
        sorted_cells = sorted_cells.reshape(chunk // 16, 2, 8, LANES)
        side = lax.broadcasted_iota(jnp.int32, (chunk // 16, 8, LANES), 2)
        out[row // 16 : (row + chunk) // 16, 16:24] = jnp.where(
            side < LANES // 2, sorted_cells[:, 0], sorted_cells[:, 1]
        )
    fetch_table.wait()
    fetch_fields.wait()
    coeffs = dot(dot(table[...], first[:NZ]), sort_fields[...])
    mode = lax.broadcasted_iota(jnp.int32, (MODES, LANES), 0)
    number = jnp.where(mode < HALF, mode, mode - HALF + 1)
    plane = lanes_of(MODES) % 32 % PLANES
    limit = jnp.zeros((MODES, LANES), jnp.int32)
    for p in range(PLANES):
        limit = jnp.where(plane == p, counts[1, p], limit)
    weight = jnp.where(mode == 0, 1.0 / NZ, 2.0 / NZ)
    coeffs = jnp.where(number <= limit, coeffs * weight, 0.0)
    out[:, 0:16] = dot(table[...].T, coeffs).reshape(GZ, 16, LANES)


def forward_body(cells, out):
    for row in range(TILE_Z):
        out[row] = cells[:, row, :]


def unsort():
    source = lax.broadcasted_iota(jnp.int32, (LANES, LANES), 0)
    target = lax.broadcasted_iota(jnp.int32, (LANES, LANES), 1)
    return jnp.where(target == source % 32 * 4 + source // 32, 1.0, 0.0)


def cells_body(cells, out, rows):
    lane = lanes_of(16)
    order = unsort()
    for group in range(2):
        stacked = jnp.concatenate(
            [cells[:, 16 + 4 * group + r, :] for r in range(4)], axis=0
        )
        turned = stacked.T
        for half in range(2):
            for r in range(4):
                joined = jnp.zeros((16, LANES), jnp.float32)
                for column in range(4):
                    begin = half * 64 + column * 16
                    moved = roll(turned[begin : begin + 16], (column - r) * 32, 1)
                    joined = jnp.where(lane // 32 == column, moved, joined)
                place = (half * 8 + group * 4 + r) * 16
                rows[place : place + 16] = joined
    rows[...] = dot(rows[...], order)
    for c in range(3):
        for p in range(PLANES):
            out[c, p] = rows[pl.ds(c * PLANES + p, TILE_Z, stride=16), :]


def streamwise_body(counts, lines, far_table, out, rows, table, done):
    fetches = [
        pltpu.make_async_copy(far_table.at[column], table.at[column], done.at[column])
        for column in range(4)
    ]
    for fetch in fetches:
        fetch.start()
    cells = lines[...].reshape(NX // 4, LANES)
    fetches[0].wait()
    coeffs = dot(table[0], cells)
    for column in range(1, 4):
        fetches[column].wait()
        coeffs = coeffs + roll(dot(table[column], cells), -32 * column, 1)
    mode = lax.broadcasted_iota(jnp.int32, (MODES, LANES), 0)
    number = jnp.where(mode < HALF, mode, mode - HALF + 1)
    weight = jnp.where(mode == 0, 1.0 / NX, 2.0 / NX)
    lane = lanes_of(MODES)
    limit = jnp.full((MODES, LANES), -1, jnp.int32)
    for p in range(PLANES):
        limit = jnp.where((lane < 27) & (lane % PLANES == p), counts[0, p], limit)
    coeffs = jnp.where(number <= limit, coeffs * weight, 0.0).T[:32]
    rows[...] = jnp.zeros(rows.shape, jnp.float32)
    for column in range(4):
        filtered = dot(coeffs, table[column])
        for q, (a, b) in enumerate(zip(pair_first, pair_second)):
            rows[column, 3 * q : 3 * q + 3] = (
                filtered[9 + 3 * q : 12 + 3 * q]
                - filtered[3 * a : 3 * a + 3] * filtered[3 * b : 3 * b + 3]
            )
    lane = lanes_of(24)
    for dest in range(GX):
        begin = dest // 4 * LANES
        joined = jnp.zeros((24, LANES), jnp.float32)
        for column in range(4):
            moved = roll(rows[column, :, begin : begin + LANES], (column - dest % 4) * 32, 1)
            joined = jnp.where(lane // 32 == column, moved, joined)
        out[dest] = joined


def stress_body(lines, out, rows):
    rows[...] = dot(lines[...].reshape(16 * 24, LANES), unsort())
    for q in range(6):
        for p in range(PLANES):
            out[q, p] = rows[pl.ds(q * PLANES + p, TILE_Z, stride=24), :]


def wave_table(length):
    column = np.arange(MODES)
    numbers = np.where(column < HALF, column, column - HALF + 1)
    angles = (np.arange(length)[:, None] * numbers[None, :] % length) * (2.0 * math.pi / length)
    return np.where(column[None, :] < HALF, np.cos(angles), np.sin(angles))


def wave_tables():
    synth_z = wave_table(NZ).T
    synth_x = wave_table(NX).reshape(NX // 4, 4, MODES).transpose(1, 2, 0)
    sort_fields = np.zeros((LANES, LANES))
    sort_cells = np.zeros((LANES, LANES))
    kinds = ((0, 1, 2), (3, 6, 8), (4, 7, 5))
    for c in range(3):
        for p in range(PLANES):
            for column in range(4):
                lane = c * STRIDE + p * SLOT + 3 + column
                for kind in range(3):
                    field = kinds[kind][c] * PLANES + p
                    sort_fields[lane + 4 * kind, column * 32 + field] = 1.0
                for half in range(2):
                    sort_cells[lane, half * 64 + column * 16 + c * PLANES + p] = 1.0
    return [
        jnp.asarray(np.ascontiguousarray(values, dtype=np.float32))
        for values in (synth_z, sort_fields, sort_cells, synth_x)
    ]


def local(velocity, downflow, shear, mode_counts):
    count = lax.axis_size("gx")
    mode_counts = mode_counts.T
    left = lax.ppermute(velocity, "gx", [(i, (i + 1) % count) for i in range(count)])
    right = lax.ppermute(velocity, "gx", [((i + 1) % count, i) for i in range(count)])
    synth_z, sort_fields, sort_cells, synth_x = wave_tables()
    (inner,) = call(inner_body, [(GZ, TILE_Z, LANES)], 0, [], velocity)
    (cells,) = call(
        outer_body,
        [(GZ, TILE_Z, LANES)],
        0,
        [],
        velocity,
        left,
        right,
        inner,
        alias={3: 0},
    )
    cells = lax.all_to_all(cells, spanwise, 0, 0, tiled=True)
    (cells,) = call(
        advance_body,
        [(GZ, 24, LANES)],
        3,
        [(NZ + 16, LANES)] * 3,
        downflow,
        shear,
        mode_counts,
        cells,
        synth_z,
        sort_fields,
        sort_cells,
        tables=3,
    )
    cells = lax.all_to_all(cells, spanwise, 0, 0, tiled=True)
    (lines,) = call(forward_body, [(GX, GZ, LANES)], 0, [], cells)
    lines = lax.all_to_all(lines, "gx", 0, 0, tiled=True)
    (advanced,) = call(
        cells_body, [(3, PLANES, TILE_Z, TILE_X)], 0, [(16 * TILE_Z, LANES)], cells, final=True
    )
    (lines,) = call(
        streamwise_body,
        [(GX, 24, LANES)],
        1,
        [(4, 24, NX // 4)],
        mode_counts,
        lines,
        synth_x,
        tables=1,
    )
    lines = lax.all_to_all(lines, "gx", 0, 0, tiled=True)
    (stress,) = call(
        stress_body, [(6, PLANES, TILE_Z, TILE_X)], 0, [(16 * 24, LANES)], lines, final=True
    )
    return advanced, stress


def solution(mesh):
    return jax.shard_map(
        local,
        mesh=mesh,
        in_specs=(P(None, None, ("gz", "grp"), "gx"), P(), P(), P()),
        out_specs=(P(None, None, ("gz", "grp"), "gx"), P(None, None, ("gz", "grp"), "gx")),
        check_vma=False,
    )
```

```python
import math

import jax
import jax.numpy as jnp
import numpy as np
from jax import lax
from jax.experimental import pallas as pl
from jax.experimental.pallas import tpu as pltpu
from jax.sharding import PartitionSpec as P

NX = 2048
NZ = 512
MODES = 256
HALF = MODES // 2
PLANES = 3
TILE_Z = 16
TILE_X = 128
GX = NX // TILE_X
GZ = NZ // TILE_Z
LANES = 128

SLOT = 14
STRIDE = PLANES * SLOT

molecular_diffusivity = 0.4
time_step = 0.2
spanwise = ("gz", "grp")
pair_first = (0, 0, 0, 1, 1, 2)
pair_second = (0, 1, 2, 1, 2, 2)


def roll(values, shift, axis):
    shift = shift % values.shape[axis]
    return pltpu.roll(values, shift, axis) if shift else values


def call(body, out_shapes, smem, scratch, *args, tables=0, final=False, alias=None):
    make = jax.ShapeDtypeStruct if final else pltpu.VMEM
    near = len(args) - tables
    args = (
        args[:smem]
        + tuple(pltpu.with_memory_space_constraint(arg, pltpu.VMEM) for arg in args[smem:near])
        + args[near:]
    )
    fetched = [pltpu.VMEM(arg.shape, arg.dtype) for arg in args[near:]]
    return pl.pallas_call(
        body,
        out_shape=[make(shape, jnp.float32) for shape in out_shapes],
        in_specs=[pl.BlockSpec(memory_space=pltpu.SMEM)] * smem
        + [pl.BlockSpec(memory_space=pltpu.VMEM)] * (near - smem)
        + [pl.BlockSpec(memory_space=pl.ANY)] * tables,
        out_specs=[pl.BlockSpec(memory_space=pltpu.VMEM)] * len(out_shapes),
        scratch_shapes=[pltpu.VMEM(shape, jnp.float32) for shape in scratch]
        + fetched
        + ([pltpu.SemaphoreType.DMA((4,))] if tables else []),
        input_output_aliases=alias or {},
    )(*args)


def dot(left, right):
    return lax.dot_general(
        left,
        right,
        (((1,), (0,)), ((), ())),
        precision=lax.Precision.DEFAULT,
        preferred_element_type=jnp.float32,
    )


def parts(values, count):
    terms = []
    for index in range(count):
        terms.append(values.astype(jnp.bfloat16))
        if index + 1 < count:
            values = values - terms[-1].astype(jnp.float32)
    return terms


def picked(values, choice):
    rows = values.shape[0]
    sums = dot(jnp.concatenate(parts(values, 3), axis=0), choice)
    return sums[:rows] + (sums[rows : 2 * rows] + sums[2 * rows :])


def table_dot(high, low, values):
    width = values.shape[1]
    large, small = parts(values, 2)
    sums = dot(high, jnp.concatenate([large, small], axis=1))
    return sums[:, :width] + (sums[:, width:] + dot(low, large))


def dot_table(values, high, low):
    rows = values.shape[0]
    large, small = parts(values, 2)
    sums = dot(jnp.concatenate([large, small], axis=0), high)
    return sums[:rows] + (sums[rows:] + dot(large, low))


def lanes_of(rows):
    return lax.broadcasted_iota(jnp.int32, (rows, LANES), 1)


def packed_for(dest, sides):
    lane = lanes_of(TILE_Z)
    packed = jnp.zeros((TILE_Z, LANES), jnp.float32)
    for index, values in enumerate(sides):
        moved = roll(values, index * SLOT - (4 * dest - 3), 1)
        here = (lane >= index * SLOT) & (lane < index * SLOT + 10)
        packed = jnp.where(here, moved, packed)
    return packed


def inner_body(own, out):
    cells = [own[c, p] for c in range(3) for p in range(PLANES)]
    for dest in range(1, GZ - 1):
        out[dest] = packed_for(dest, cells)
    out[0] = packed_for(GZ // 2, cells)
    out[GZ - 1] = packed_for(GZ // 2, cells)


def outer_body(own, left, right, inner, out):
    low = lanes_of(TILE_Z) < LANES // 2
    pairs = [(c, p) for c in range(3) for p in range(PLANES)]
    out[0] = packed_for(0, [jnp.where(low, own[c, p], left[c, p]) for c, p in pairs])
    out[GZ - 1] = packed_for(
        GZ - 1, [jnp.where(low, right[c, p], own[c, p]) for c, p in pairs]
    )


def advance_body(
    downflow, shear, counts, cells, far_table, far_synth, far_fields, far_cells,
    out, start, first, second, table, synth, sort_fields, sort_cells, done,
):
    fetch_table = pltpu.make_async_copy(far_table, table, done.at[0])
    fetch_fields = pltpu.make_async_copy(far_fields, sort_fields, done.at[1])
    fetch_cells = pltpu.make_async_copy(far_cells, sort_cells, done.at[2])
    fetch_synth = pltpu.make_async_copy(far_synth, synth, done.at[3])
    fetch_cells.start()
    fetch_table.start()
    fetch_fields.start()
    fetch_synth.start()
    chunk = 64
    edge = 8
    lane = lanes_of(chunk)
    component = lane // STRIDE
    plane = lane % STRIDE // SLOT
    flow = jnp.zeros((chunk, LANES), jnp.float32)
    slope = jnp.zeros((chunk, LANES), jnp.float32)
    for p in range(PLANES):
        flow = jnp.where(plane == p, downflow[p], flow)
        slope = jnp.where((plane == p) & (component == 0), shear[p], slope)

    def store(ref, row, values):
        ref[edge + row : edge + row + chunk] = values
        if row == 0:
            ref[edge + NZ : edge + NZ + edge] = values[:edge]
        if row == NZ - chunk:
            ref[:edge] = values[chunk - edge :]

    def rate(ref, row):
        low = edge + row
        middle = ref[low : low + chunk]
        north = ref[low + 1 : low + 1 + chunk]
        south = ref[low - 1 : low - 1 + chunk]
        east = roll(middle, -1, 1)
        west = roll(middle, 1, 1)
        next_one = roll(middle, -STRIDE, 1)
        along = jnp.where(
            component == 0,
            middle,
            jnp.where(component == 1, roll(middle, STRIDE, 1), roll(middle, 2 * STRIDE, 1)),
        )
        across = jnp.where(
            component == 2,
            middle,
            jnp.where(component == 1, next_one, roll(middle, -2 * STRIDE, 1)),
        )
        return middle, (
            -(flow + along) * ((east - west) * 0.5)
            - across * ((north - south) * 0.5)
            + molecular_diffusivity * (east + west + north + south - 4.0 * middle)
            - slope * next_one
        )

    rows = range(0, NZ, chunk)
    for row in rows:
        store(start, row, cells[row // 16 : (row + chunk) // 16].reshape(chunk, LANES))
    for row in rows:
        middle, change = rate(start, row)
        store(first, row, middle + time_step * change)
    for row in rows:
        middle, change = rate(first, row)
        begin = start[edge + row : edge + row + chunk]
        store(second, row, 0.75 * begin + 0.25 * (middle + time_step * change))
    fetch_cells.wait()
    part = (lane + LANES - 3) % LANES % SLOT // 4
    part = jnp.where((lane >= 3) & (lane < 127), part, 3)
    for row in rows:
        middle, change = rate(second, row)
        begin = start[edge + row : edge + row + chunk]
        last = begin * (1.0 / 3.0) + (2.0 / 3.0) * (middle + time_step * change)
        other = jnp.where(component == 2, roll(last, 2 * STRIDE, 1), roll(last, -STRIDE, 1))
        fields = jnp.where(part == 0, last, 0.0)
        fields = jnp.where(part == 1, roll(last * last, 4, 1), fields)
        first[row : row + chunk] = jnp.where(part == 2, roll(last * other, 8, 1), fields)
        sorted_cells = picked(jnp.where(part == 0, last, 0.0), sort_cells[...])
        sorted_cells = sorted_cells.reshape(chunk // 16, 2, 8, LANES)
        side = lax.broadcasted_iota(jnp.int32, (chunk // 16, 8, LANES), 2)
        out[row // 16 : (row + chunk) // 16, 16:24] = jnp.where(
            side < LANES // 2, sorted_cells[:, 0], sorted_cells[:, 1]
        )
    fetch_table.wait()
    fetch_fields.wait()
    coeffs = picked(table_dot(table[0], table[1], first[:NZ]), sort_fields[...])
    mode = lax.broadcasted_iota(jnp.int32, (MODES, LANES), 0)
    number = jnp.where(mode < HALF, mode, mode - HALF + 1)
    plane = lanes_of(MODES) % 32 % PLANES
    limit = jnp.zeros((MODES, LANES), jnp.int32)
    for p in range(PLANES):
        limit = jnp.where(plane == p, counts[1, p], limit)
    weight = jnp.where(mode == 0, 1.0 / NZ, 2.0 / NZ)
    coeffs = jnp.where(number <= limit, coeffs * weight, 0.0)
    fetch_synth.wait()
    out[:, 0:16] = table_dot(synth[0], synth[1], coeffs).reshape(GZ, 16, LANES)


def forward_body(cells, out):
    for row in range(TILE_Z):
        out[row] = cells[:, row, :]


def unsort():
    source = lax.broadcasted_iota(jnp.int32, (LANES, LANES), 0)
    target = lax.broadcasted_iota(jnp.int32, (LANES, LANES), 1)
    return jnp.where(target == source % 32 * 4 + source // 32, 1.0, 0.0).astype(jnp.bfloat16)


def cells_body(cells, out, rows):
    lane = lanes_of(16)
    order = unsort()
    for group in range(2):
        stacked = jnp.concatenate(
            [cells[:, 16 + 4 * group + r, :] for r in range(4)], axis=0
        )
        turned = stacked.T
        for half in range(2):
            for r in range(4):
                joined = jnp.zeros((16, LANES), jnp.float32)
                for column in range(4):
                    begin = half * 64 + column * 16
                    moved = roll(turned[begin : begin + 16], (column - r) * 32, 1)
                    joined = jnp.where(lane // 32 == column, moved, joined)
                place = (half * 8 + group * 4 + r) * 16
                rows[place : place + 16] = joined
    rows[...] = picked(rows[...], order)
    for c in range(3):
        for p in range(PLANES):
            out[c, p] = rows[pl.ds(c * PLANES + p, TILE_Z, stride=16), :]


def streamwise_body(counts, lines, far_table, out, rows, table, done):
    fetches = [
        pltpu.make_async_copy(far_table.at[column], table.at[column], done.at[column])
        for column in range(4)
    ]
    for fetch in fetches:
        fetch.start()
    cells = lines[...].reshape(NX // 4, LANES)
    fetches[0].wait()
    coeffs = table_dot(table[0, 0], table[0, 1], cells)
    for column in range(1, 4):
        fetches[column].wait()
        coeffs = coeffs + roll(
            table_dot(table[column, 0], table[column, 1], cells), -32 * column, 1
        )
    mode = lax.broadcasted_iota(jnp.int32, (MODES, LANES), 0)
    number = jnp.where(mode < HALF, mode, mode - HALF + 1)
    weight = jnp.where(mode == 0, 1.0 / NX, 2.0 / NX)
    lane = lanes_of(MODES)
    limit = jnp.full((MODES, LANES), -1, jnp.int32)
    for p in range(PLANES):
        limit = jnp.where((lane < 27) & (lane % PLANES == p), counts[0, p], limit)
    coeffs = jnp.where(number <= limit, coeffs * weight, 0.0).T[:32]
    rows[...] = jnp.zeros(rows.shape, jnp.float32)
    for column in range(4):
        filtered = dot_table(coeffs, table[column, 0], table[column, 1])
        for q, (a, b) in enumerate(zip(pair_first, pair_second)):
            rows[column, 3 * q : 3 * q + 3] = (
                filtered[9 + 3 * q : 12 + 3 * q]
                - filtered[3 * a : 3 * a + 3] * filtered[3 * b : 3 * b + 3]
            )
    lane = lanes_of(24)
    for dest in range(GX):
        begin = dest // 4 * LANES
        joined = jnp.zeros((24, LANES), jnp.float32)
        for column in range(4):
            moved = roll(rows[column, :, begin : begin + LANES], (column - dest % 4) * 32, 1)
            joined = jnp.where(lane // 32 == column, moved, joined)
        out[dest] = joined


def stress_body(lines, out, rows):
    rows[...] = picked(lines[...].reshape(16 * 24, LANES), unsort())
    for q in range(6):
        for p in range(PLANES):
            out[q, p] = rows[pl.ds(q * PLANES + p, TILE_Z, stride=24), :]


def wave_table(length):
    column = np.arange(MODES)
    numbers = np.where(column < HALF, column, column - HALF + 1)
    angles = (np.arange(length)[:, None] * numbers[None, :] % length) * (2.0 * math.pi / length)
    return np.where(column[None, :] < HALF, np.cos(angles), np.sin(angles))


def wave_tables():
    synth_z = wave_table(NZ).T
    synth_x = wave_table(NX).reshape(NX // 4, 4, MODES).transpose(1, 2, 0)
    sort_fields = np.zeros((LANES, LANES))
    sort_cells = np.zeros((LANES, LANES))
    kinds = ((0, 1, 2), (3, 6, 8), (4, 7, 5))
    for c in range(3):
        for p in range(PLANES):
            for column in range(4):
                lane = c * STRIDE + p * SLOT + 3 + column
                for kind in range(3):
                    field = kinds[kind][c] * PLANES + p
                    sort_fields[lane + 4 * kind, column * 32 + field] = 1.0
                for half in range(2):
                    sort_cells[lane, half * 64 + column * 16 + c * PLANES + p] = 1.0

    def halves(values):
        high = values.astype(jnp.bfloat16)
        low = (values - high.astype(np.float64)).astype(jnp.bfloat16)
        return np.stack([high, low], axis=-3)

    return [
        jnp.asarray(np.ascontiguousarray(values))
        for values in (
            halves(synth_z),
            halves(synth_z.T),
            sort_fields.astype(jnp.bfloat16),
            sort_cells.astype(jnp.bfloat16),
            halves(synth_x),
        )
    ]


def local(velocity, downflow, shear, mode_counts):
    count = lax.axis_size("gx")
    mode_counts = mode_counts.T
    left = lax.ppermute(velocity, "gx", [(i, (i + 1) % count) for i in range(count)])
    right = lax.ppermute(velocity, "gx", [((i + 1) % count, i) for i in range(count)])
    analysis_z, synth_z, sort_fields, sort_cells, synth_x = wave_tables()
    (inner,) = call(inner_body, [(GZ, TILE_Z, LANES)], 0, [], velocity)
    (cells,) = call(
        outer_body,
        [(GZ, TILE_Z, LANES)],
        0,
        [],
        velocity,
        left,
        right,
        inner,
        alias={3: 0},
    )
    cells = lax.all_to_all(cells, spanwise, 0, 0, tiled=True)
    (cells,) = call(
        advance_body,
        [(GZ, 24, LANES)],
        3,
        [(NZ + 16, LANES)] * 3,
        downflow,
        shear,
        mode_counts,
        cells,
        analysis_z,
        synth_z,
        sort_fields,
        sort_cells,
        tables=4,
    )
    cells = lax.all_to_all(cells, spanwise, 0, 0, tiled=True)
    (lines,) = call(forward_body, [(GX, GZ, LANES)], 0, [], cells)
    lines = lax.all_to_all(lines, "gx", 0, 0, tiled=True)
    (advanced,) = call(
        cells_body, [(3, PLANES, TILE_Z, TILE_X)], 0, [(16 * TILE_Z, LANES)], cells, final=True
    )
    (lines,) = call(
        streamwise_body,
        [(GX, 24, LANES)],
        1,
        [(4, 24, NX // 4)],
        mode_counts,
        lines,
        synth_x,
        tables=1,
    )
    lines = lax.all_to_all(lines, "gx", 0, 0, tiled=True)
    (stress,) = call(
        stress_body, [(6, PLANES, TILE_Z, TILE_X)], 0, [(16 * 24, LANES)], lines, final=True
    )
    return advanced, stress


def solution(mesh):
    return jax.shard_map(
        local,
        mesh=mesh,
        in_specs=(P(None, None, ("gz", "grp"), "gx"), P(), P(), P()),
        out_specs=(P(None, None, ("gz", "grp"), "gx"), P(None, None, ("gz", "grp"), "gx")),
        check_vma=False,
    )
```

```python
import math

import jax
import jax.numpy as jnp
import numpy as np
from jax import lax
from jax.experimental import pallas as pl
from jax.experimental.pallas import tpu as pltpu
from jax.sharding import PartitionSpec as P

NX = 2048
NZ = 512
MODES = 256
HALF = MODES // 2
PLANES = 3
TILE_Z = 16
TILE_X = 128
GX = NX // TILE_X
GZ = NZ // TILE_Z
LANES = 128

SLOT = 14
STRIDE = PLANES * SLOT
FIELDS = 9 * PLANES
BACK = 18
STRESSES = 6 * PLANES

molecular_diffusivity = 0.4
time_step = 0.2
spanwise = ("gz", "grp")
pair_first = (0, 0, 0, 1, 1, 2)
pair_second = (0, 1, 2, 1, 2, 2)


def roll(values, shift, axis):
    shift = shift % values.shape[axis]
    return pltpu.roll(values, shift, axis) if shift else values


def call(body, out_shapes, smem, scratch, *args, tables=0, final=False, alias=None):
    make = jax.ShapeDtypeStruct if final else pltpu.VMEM
    near = len(args) - tables
    args = (
        args[:smem]
        + tuple(pltpu.with_memory_space_constraint(arg, pltpu.VMEM) for arg in args[smem:near])
        + args[near:]
    )
    fetched = [pltpu.VMEM(arg.shape, arg.dtype) for arg in args[near:]]
    return pl.pallas_call(
        body,
        out_shape=[make(shape, jnp.float32) for shape in out_shapes],
        in_specs=[pl.BlockSpec(memory_space=pltpu.SMEM)] * smem
        + [pl.BlockSpec(memory_space=pltpu.VMEM)] * (near - smem)
        + [pl.BlockSpec(memory_space=pl.ANY)] * tables,
        out_specs=[pl.BlockSpec(memory_space=pltpu.VMEM)] * len(out_shapes),
        scratch_shapes=[pltpu.VMEM(shape, jnp.float32) for shape in scratch]
        + fetched
        + ([pltpu.SemaphoreType.DMA((4,))] if tables else []),
        input_output_aliases=alias or {},
    )(*args)


def dot(left, right):
    return lax.dot_general(
        left,
        right,
        (((1,), (0,)), ((), ())),
        precision=lax.Precision.DEFAULT,
        preferred_element_type=jnp.float32,
    )


def parts(values, count):
    terms = []
    for index in range(count):
        terms.append(values.astype(jnp.bfloat16))
        if index + 1 < count:
            values = values - terms[-1].astype(jnp.float32)
    return terms


def picked(values, choice):
    rows = values.shape[0]
    sums = dot(jnp.concatenate(parts(values, 3), axis=0), choice)
    return sums[:rows] + (sums[rows : 2 * rows] + sums[2 * rows :])


def table_dot(high, low, values):
    width = values.shape[1]
    large, small = parts(values, 2)
    sums = dot(high, jnp.concatenate([large, small], axis=1))
    return sums[:, :width] + (sums[:, width:] + dot(low, large))


def dot_table(values, high, low):
    rows = values.shape[0]
    large, small = parts(values, 2)
    sums = dot(jnp.concatenate([large, small], axis=0), high)
    return sums[:rows] + (sums[rows:] + dot(large, low))


def lanes_of(rows):
    return lax.broadcasted_iota(jnp.int32, (rows, LANES), 1)


def packed_for(dest, sides):
    lane = lanes_of(TILE_Z)
    packed = jnp.zeros((TILE_Z, LANES), jnp.float32)
    for index, values in enumerate(sides):
        moved = roll(values, index * SLOT - (4 * dest - 3), 1)
        here = (lane >= index * SLOT) & (lane < index * SLOT + 10)
        packed = jnp.where(here, moved, packed)
    return packed


def inner_body(own, out):
    cells = [own[c, p] for c in range(3) for p in range(PLANES)]
    for dest in range(1, GZ - 1):
        out[dest] = packed_for(dest, cells)
    out[0] = packed_for(GZ // 2, cells)
    out[GZ - 1] = packed_for(GZ // 2, cells)


def outer_body(own, left, right, inner, out):
    low = lanes_of(TILE_Z) < LANES // 2
    pairs = [(c, p) for c in range(3) for p in range(PLANES)]
    out[0] = packed_for(0, [jnp.where(low, own[c, p], left[c, p]) for c, p in pairs])
    out[GZ - 1] = packed_for(
        GZ - 1, [jnp.where(low, right[c, p], own[c, p]) for c, p in pairs]
    )


def advance_body(
    downflow, shear, counts, cells, far_table, far_synth, far_fields, far_cells,
    out, start, first, second, table, synth, sort_fields, sort_cells, done,
):
    fetch_table = pltpu.make_async_copy(far_table, table, done.at[0])
    fetch_fields = pltpu.make_async_copy(far_fields, sort_fields, done.at[1])
    fetch_cells = pltpu.make_async_copy(far_cells, sort_cells, done.at[2])
    fetch_synth = pltpu.make_async_copy(far_synth, synth, done.at[3])
    fetch_cells.start()
    fetch_table.start()
    fetch_fields.start()
    fetch_synth.start()
    chunk = 64
    edge = 8
    lane = lanes_of(chunk)
    component = lane // STRIDE
    plane = lane % STRIDE // SLOT
    flow = jnp.zeros((chunk, LANES), jnp.float32)
    slope = jnp.zeros((chunk, LANES), jnp.float32)
    for p in range(PLANES):
        flow = jnp.where(plane == p, downflow[p], flow)
        slope = jnp.where((plane == p) & (component == 0), shear[p], slope)

    def store(ref, row, values):
        ref[edge + row : edge + row + chunk] = values
        if row == 0:
            ref[edge + NZ : edge + NZ + edge] = values[:edge]
        if row == NZ - chunk:
            ref[:edge] = values[chunk - edge :]

    def rate(ref, row):
        low = edge + row
        middle = ref[low : low + chunk]
        north = ref[low + 1 : low + 1 + chunk]
        south = ref[low - 1 : low - 1 + chunk]
        east = roll(middle, -1, 1)
        west = roll(middle, 1, 1)
        next_one = roll(middle, -STRIDE, 1)
        along = jnp.where(
            component == 0,
            middle,
            jnp.where(component == 1, roll(middle, STRIDE, 1), roll(middle, 2 * STRIDE, 1)),
        )
        across = jnp.where(
            component == 2,
            middle,
            jnp.where(component == 1, next_one, roll(middle, -2 * STRIDE, 1)),
        )
        return middle, (
            -(flow + along) * ((east - west) * 0.5)
            - across * ((north - south) * 0.5)
            + molecular_diffusivity * (east + west + north + south - 4.0 * middle)
            - slope * next_one
        )

    rows = range(0, NZ, chunk)
    for row in rows:
        store(start, row, cells[row // 16 : (row + chunk) // 16].reshape(chunk, LANES))
    for row in rows:
        middle, change = rate(start, row)
        store(first, row, middle + time_step * change)
    for row in rows:
        middle, change = rate(first, row)
        begin = start[edge + row : edge + row + chunk]
        store(second, row, 0.75 * begin + 0.25 * (middle + time_step * change))
    in_eight = lax.broadcasted_iota(jnp.int32, (chunk, LANES), 0) % 8
    fetch_cells.wait()
    part = (lane + LANES - 3) % LANES % SLOT // 4
    part = jnp.where((lane >= 3) & (lane < 127), part, 3)
    for row in rows:
        middle, change = rate(second, row)
        begin = start[edge + row : edge + row + chunk]
        last = begin * (1.0 / 3.0) + (2.0 / 3.0) * (middle + time_step * change)
        other = jnp.where(component == 2, roll(last, 2 * STRIDE, 1), roll(last, -STRIDE, 1))
        fields = jnp.where(part == 0, last, 0.0)
        fields = jnp.where(part == 1, roll(last * last, 4, 1), fields)
        first[row : row + chunk] = jnp.where(part == 2, roll(last * other, 8, 1), fields)
        sorted_cells = picked(jnp.where(part == 0, last, 0.0), sort_cells[...])
        start[edge + row : edge + row + chunk] = sorted_cells[:, :LANES]
        rest = jnp.where(lane // 16 == in_eight, sorted_cells[:, LANES:], 0.0)
        rest = jnp.sum(rest.reshape(chunk // 8, 8, LANES), axis=1)
        for block in range(chunk // 16):
            place = (row // 16 + block) * BACK + 16
            out[place : place + 2] = rest[2 * block : 2 * block + 2]
    fetch_table.wait()
    fetch_fields.wait()
    coeffs = picked(table_dot(table[0], table[1], first[:NZ]), sort_fields[...])
    mode = lax.broadcasted_iota(jnp.int32, (MODES, LANES), 0)
    number = jnp.where(mode < HALF, mode, mode - HALF + 1)
    plane = lanes_of(MODES) % PLANES
    limit = jnp.zeros((MODES, LANES), jnp.int32)
    for p in range(PLANES):
        limit = jnp.where(plane == p, counts[1, p], limit)
    weight = jnp.where(mode == 0, 1.0 / NZ, 2.0 / NZ)
    coeffs = jnp.where(number <= limit, coeffs * weight, 0.0)
    fetch_synth.wait()
    filtered = table_dot(synth[0], synth[1], coeffs) + start[edge : edge + NZ]
    for block in range(GZ):
        out[block * BACK : block * BACK + 16] = filtered[16 * block : 16 * block + 16]


def forward_body(cells, out):
    for row in range(TILE_Z):
        out[row] = cells[pl.ds(row, GZ, stride=BACK), :]


def unsort():
    source = lax.broadcasted_iota(jnp.int32, (LANES, LANES), 0)
    target = lax.broadcasted_iota(jnp.int32, (LANES, LANES), 1)
    return jnp.where(target == source % 32 * 4 + source // 32, 1.0, 0.0).astype(jnp.bfloat16)


def cells_body(cells, out, rows):
    lane = lanes_of(8)
    rest = jnp.concatenate(
        [cells[pl.ds(16 + half, GZ, stride=BACK), :] for half in range(2)] * 2, axis=0
    ).T
    for group in range(4):
        turned = jnp.concatenate(
            [cells[pl.ds(4 * group + r, GZ, stride=BACK), :] for r in range(4)], axis=0
        ).T
        for r in range(4):
            row = 4 * group + r
            for begin, source, count, at in (
                (4 * FIELDS, turned, 5, r),
                (row % 8 * 16, rest, 4, row // 8),
            ):
                joined = jnp.zeros((count, LANES), jnp.float32)
                for column in range(4):
                    low = begin + column * count
                    moved = roll(source[low : low + count], (column - at) * 32, 1)
                    joined = jnp.where(lane[:count] // 32 == column, moved, joined)
                place = row * 16 + (0 if count == 5 else 5)
                rows[place : place + count] = joined
            rows[row * 16 + 9 : row * 16 + 16] = jnp.zeros((7, LANES), jnp.float32)
    order = unsort()
    rows[...] = picked(rows[...], order)
    for c in range(3):
        for p in range(PLANES):
            out[c, p] = rows[pl.ds(c * PLANES + p, TILE_Z, stride=16), :]


def streamwise_body(counts, lines, far_table, out, rows, table, done):
    fetches = [
        pltpu.make_async_copy(far_table.at[column], table.at[column], done.at[column])
        for column in range(4)
    ]
    for fetch in fetches:
        fetch.start()
    cells = lines[...].reshape(NX // 4, LANES)
    fetches[0].wait()
    coeffs = table_dot(table[0, 0], table[0, 1], cells)
    for column in range(1, 4):
        fetches[column].wait()
        coeffs = coeffs + roll(
            table_dot(table[column, 0], table[column, 1], cells), -FIELDS * column, 1
        )
    mode = lax.broadcasted_iota(jnp.int32, (MODES, LANES), 0)
    number = jnp.where(mode < HALF, mode, mode - HALF + 1)
    weight = jnp.where(mode == 0, 1.0 / NX, 2.0 / NX)
    lane = lanes_of(MODES)
    limit = jnp.full((MODES, LANES), -1, jnp.int32)
    for p in range(PLANES):
        limit = jnp.where((lane < FIELDS) & (lane % PLANES == p), counts[0, p], limit)
    coeffs = jnp.where(number <= limit, coeffs * weight, 0.0).T[:32]
    rows[...] = jnp.zeros(rows.shape, jnp.float32)
    for column in range(4):
        filtered = dot_table(coeffs, table[column, 0], table[column, 1])
        for q, (a, b) in enumerate(zip(pair_first, pair_second)):
            rows[column, 3 * q : 3 * q + 3] = (
                filtered[9 + 3 * q : 12 + 3 * q]
                - filtered[3 * a : 3 * a + 3] * filtered[3 * b : 3 * b + 3]
            )
    lane = lanes_of(24)
    for dest in range(GX):
        begin = dest // 4 * LANES
        joined = jnp.zeros((24, LANES), jnp.float32)
        for column in range(4):
            moved = roll(rows[column, :, begin : begin + LANES], (column - dest % 4) * 32, 1)
            joined = jnp.where(lane // 32 == column, moved, joined)
        out[dest * STRESSES : (dest + 1) * STRESSES] = joined[:STRESSES]


def stress_body(lines, out, rows):
    rows[...] = picked(lines[...], unsort())
    for q in range(6):
        for p in range(PLANES):
            out[q, p] = rows[pl.ds(q * PLANES + p, TILE_Z, stride=STRESSES), :]


def wave_table(length):
    column = np.arange(MODES)
    numbers = np.where(column < HALF, column, column - HALF + 1)
    angles = (np.arange(length)[:, None] * numbers[None, :] % length) * (2.0 * math.pi / length)
    return np.where(column[None, :] < HALF, np.cos(angles), np.sin(angles))


def wave_tables():
    synth_z = wave_table(NZ).T
    synth_x = wave_table(NX).reshape(NX // 4, 4, MODES).transpose(1, 2, 0)
    sort_fields = np.zeros((LANES, LANES))
    sort_cells = np.zeros((LANES, 2 * LANES))
    kinds = ((0, 1, 2), (3, 6, 8), (4, 7, 5))
    for c in range(3):
        for p in range(PLANES):
            for column in range(4):
                lane = c * STRIDE + p * SLOT + 3 + column
                for kind in range(3):
                    field = kinds[kind][c] * PLANES + p
                    sort_fields[lane + 4 * kind, column * FIELDS + field] = 1.0
                index = c * PLANES + p
                if index < 5:
                    sort_cells[lane, 4 * FIELDS + column * 5 + index] = 1.0
                else:
                    begin = LANES + column * 4 + index - 5
                    sort_cells[lane, begin : 2 * LANES : 16] = 1.0

    def halves(values):
        high = values.astype(jnp.bfloat16)
        low = (values - high.astype(np.float64)).astype(jnp.bfloat16)
        return np.stack([high, low], axis=-3)

    return [
        jnp.asarray(np.ascontiguousarray(values))
        for values in (
            halves(synth_z),
            halves(synth_z.T),
            sort_fields.astype(jnp.bfloat16),
            sort_cells.astype(jnp.bfloat16),
            halves(synth_x),
        )
    ]


def exchange(rows, axis, count):
    sent = rows.reshape(count, -1, 2, LANES)
    return lax.all_to_all(sent, axis, 0, 0, tiled=True).reshape(rows.shape)


def local(velocity, downflow, shear, mode_counts):
    count = lax.axis_size("gx")
    mode_counts = mode_counts.T
    left = lax.ppermute(velocity, "gx", [(i, (i + 1) % count) for i in range(count)])
    right = lax.ppermute(velocity, "gx", [((i + 1) % count, i) for i in range(count)])
    analysis_z, synth_z, sort_fields, sort_cells, synth_x = wave_tables()
    (inner,) = call(inner_body, [(GZ, TILE_Z, LANES)], 0, [], velocity)
    (cells,) = call(
        outer_body,
        [(GZ, TILE_Z, LANES)],
        0,
        [],
        velocity,
        left,
        right,
        inner,
        alias={3: 0},
    )
    cells = lax.all_to_all(cells, spanwise, 0, 0, tiled=True)
    (cells,) = call(
        advance_body,
        [(GZ * BACK, LANES)],
        3,
        [(NZ + 16, LANES)] * 3,
        downflow,
        shear,
        mode_counts,
        cells,
        analysis_z,
        synth_z,
        sort_fields,
        sort_cells,
        tables=4,
    )
    cells = exchange(cells, spanwise, GZ)
    (lines,) = call(forward_body, [(GX, GZ, LANES)], 0, [], cells)
    lines = lax.all_to_all(lines, "gx", 0, 0, tiled=True)
    (advanced,) = call(
        cells_body, [(3, PLANES, TILE_Z, TILE_X)], 0, [(16 * TILE_Z, LANES)], cells, final=True
    )
    (lines,) = call(
        streamwise_body,
        [(GX * STRESSES, LANES)],
        1,
        [(4, 24, NX // 4)],
        mode_counts,
        lines,
        synth_x,
        tables=1,
    )
    lines = exchange(lines, "gx", GX)
    (stress,) = call(
        stress_body, [(6, PLANES, TILE_Z, TILE_X)], 0, [(GX * STRESSES, LANES)], lines, final=True
    )
    return advanced, stress


def solution(mesh):
    return jax.shard_map(
        local,
        mesh=mesh,
        in_specs=(P(None, None, ("gz", "grp"), "gx"), P(), P(), P()),
        out_specs=(P(None, None, ("gz", "grp"), "gx"), P(None, None, ("gz", "grp"), "gx")),
        check_vma=False,
    )
```

```python
import math

import jax
import jax.numpy as jnp
import numpy as np
from jax import lax
from jax.experimental import pallas as pl
from jax.experimental.pallas import tpu as pltpu
from jax.sharding import PartitionSpec as P

NX = 2048
NZ = 512
MODES = 256
HALF = MODES // 2
PLANES = 3
TILE_Z = 16
TILE_X = 128
GX = NX // TILE_X
GZ = NZ // TILE_Z
LANES = 128

SLOT = 14
STRIDE = PLANES * SLOT
FIELDS = 9 * PLANES
BACK = 18
STRESSES = 6 * PLANES

molecular_diffusivity = 0.4
time_step = 0.2
spanwise = ("gz", "grp")
pair_first = (0, 0, 0, 1, 1, 2)
pair_second = (0, 1, 2, 1, 2, 2)


def roll(values, shift, axis):
    shift = shift % values.shape[axis]
    return pltpu.roll(values, shift, axis) if shift else values


def call(body, out_shapes, smem, scratch, *args, tables=0, final=False, alias=None):
    make = jax.ShapeDtypeStruct if final else pltpu.VMEM
    near = len(args) - tables
    args = (
        tuple(pltpu.with_memory_space_constraint(arg, pltpu.HBM) for arg in args[:smem])
        + tuple(pltpu.with_memory_space_constraint(arg, pltpu.VMEM) for arg in args[smem:near])
        + tuple(pltpu.with_memory_space_constraint(arg, pltpu.HBM) for arg in args[near:])
    )
    return pl.pallas_call(
        body,
        out_shape=[
            make(shape.shape, shape.dtype)
            if isinstance(shape, jax.Array)
            else make(shape, jnp.float32)
            for shape in out_shapes
        ],
        in_specs=[pl.BlockSpec(memory_space=pltpu.SMEM)] * smem
        + [pl.BlockSpec(memory_space=pltpu.VMEM)] * (near - smem)
        + [pl.BlockSpec(memory_space=pltpu.HBM)] * tables,
        out_specs=[pl.BlockSpec(memory_space=pltpu.VMEM)] * len(out_shapes),
        scratch_shapes=[pltpu.VMEM(shape, jnp.float32) for shape in scratch]
        + ([pltpu.SemaphoreType.DMA((tables,))] if tables else []),
        compiler_params=pltpu.CompilerParams(vmem_limit_bytes=16 << 20),
        input_output_aliases=alias or {},
    )(*args)


def dot(left, right):
    return lax.dot_general(
        left,
        right,
        (((1,), (0,)), ((), ())),
        precision=lax.Precision.DEFAULT,
        preferred_element_type=jnp.float32,
    )


def parts(values, count):
    terms = []
    for index in range(count):
        terms.append(values.astype(jnp.bfloat16))
        if index + 1 < count:
            values = values - terms[-1].astype(jnp.float32)
    return terms


def picked(values, choice):
    rows = values.shape[0]
    sums = dot(jnp.concatenate(parts(values, 3), axis=0), choice)
    return sums[:rows] + (sums[rows : 2 * rows] + sums[2 * rows :])


def table_dot(high, low, values):
    width = values.shape[1]
    large, small = parts(values, 2)
    sums = dot(high, jnp.concatenate([large, small], axis=1))
    return sums[:, :width] + (sums[:, width:] + dot(low, large))


def dot_table(values, high, low):
    rows = values.shape[0]
    large, small = parts(values, 2)
    sums = dot(jnp.concatenate([large, small], axis=0), high)
    return sums[:rows] + (sums[rows:] + dot(large, low))


def lanes_of(rows):
    return lax.broadcasted_iota(jnp.int32, (rows, LANES), 1)


def packed_for(dest, sides):
    lane = lanes_of(TILE_Z)
    packed = jnp.zeros((TILE_Z, LANES), jnp.float32)
    for index, values in enumerate(sides):
        moved = roll(values, index * SLOT - (4 * dest - 3), 1)
        here = (lane >= index * SLOT) & (lane < index * SLOT + 10)
        packed = jnp.where(here, moved, packed)
    return packed


def inner_body(downflow, shear, counts, *refs):
    far = refs[:6]
    out, flow, slope, mask_z, mask_x = refs[6:11]
    near = refs[11:17]
    done = refs[17]
    fetches = [
        pltpu.make_async_copy(source, target, done.at[index])
        for index, (source, target) in enumerate(zip(far, near))
    ]
    for fetch in fetches:
        fetch.start()
    fetches[0].wait()
    cells = [near[0][c, p] for c in range(3) for p in range(PLANES)]
    for dest in range(1, GZ - 1):
        out[dest] = packed_for(dest, cells)
    out[0] = packed_for(GZ // 2, cells)
    out[GZ - 1] = packed_for(GZ // 2, cells)
    lane = lanes_of(8)
    plane = lane % STRIDE // SLOT
    speeds = jnp.zeros((8, LANES), jnp.float32)
    shears = jnp.zeros((8, LANES), jnp.float32)
    for p in range(PLANES):
        speeds = jnp.where(plane == p, downflow[p], speeds)
        shears = jnp.where((plane == p) & (lane < STRIDE), shear[p], shears)
    flow[...] = speeds
    slope[...] = shears
    mode = lax.broadcasted_iota(jnp.int32, (MODES, LANES), 0)
    number = jnp.where(mode < HALF, mode, mode - HALF + 1)
    plane = lanes_of(MODES) % PLANES
    for mask, axis, length in ((mask_z, 1, NZ), (mask_x, 0, NX)):
        limit = jnp.zeros((MODES, LANES), jnp.int32)
        for p in range(PLANES):
            limit = jnp.where(plane == p, counts[axis, p], limit)
        weight = jnp.where(mode == 0, 1.0 / length, 2.0 / length)
        mask[...] = jnp.where(number <= limit, weight, 0.0)
    for fetch in fetches[1:]:
        fetch.wait()


def outer_body(own, left, right, inner, out):
    low = lanes_of(TILE_Z) < LANES // 2
    pairs = [(c, p) for c in range(3) for p in range(PLANES)]
    out[0] = packed_for(0, [jnp.where(low, own[c, p], left[c, p]) for c, p in pairs])
    out[GZ - 1] = packed_for(
        GZ - 1, [jnp.where(low, right[c, p], own[c, p]) for c, p in pairs]
    )


def advance_body(
    cells, flow_row, slope_row, mask, table, synth, sort_fields, sort_cells,
    out, start, first, second,
):
    chunk = 64
    edge = 8
    lane = lanes_of(chunk)
    component = lane // STRIDE
    flow = jnp.broadcast_to(flow_row[:1], (chunk, LANES))
    slope = jnp.broadcast_to(slope_row[:1], (chunk, LANES))

    def store(ref, row, values):
        ref[edge + row : edge + row + chunk] = values
        if row == 0:
            ref[edge + NZ : edge + NZ + edge] = values[:edge]
        if row == NZ - chunk:
            ref[:edge] = values[chunk - edge :]

    def rate(ref, row):
        low = edge + row
        middle = ref[low : low + chunk]
        north = ref[low + 1 : low + 1 + chunk]
        south = ref[low - 1 : low - 1 + chunk]
        east = roll(middle, -1, 1)
        west = roll(middle, 1, 1)
        next_one = roll(middle, -STRIDE, 1)
        along = jnp.where(
            component == 0,
            middle,
            jnp.where(component == 1, roll(middle, STRIDE, 1), roll(middle, 2 * STRIDE, 1)),
        )
        across = jnp.where(
            component == 2,
            middle,
            jnp.where(component == 1, next_one, roll(middle, -2 * STRIDE, 1)),
        )
        return middle, (
            -(flow + along) * ((east - west) * 0.5)
            - across * ((north - south) * 0.5)
            + molecular_diffusivity * (east + west + north + south - 4.0 * middle)
            - slope * next_one
        )

    rows = range(0, NZ, chunk)
    for row in rows:
        store(start, row, cells[row // 16 : (row + chunk) // 16].reshape(chunk, LANES))
    for row in rows:
        middle, change = rate(start, row)
        store(first, row, middle + time_step * change)
    for row in rows:
        middle, change = rate(first, row)
        begin = start[edge + row : edge + row + chunk]
        store(second, row, 0.75 * begin + 0.25 * (middle + time_step * change))
    in_eight = lax.broadcasted_iota(jnp.int32, (chunk, LANES), 0) % 8
    part = (lane + LANES - 3) % LANES % SLOT // 4
    part = jnp.where((lane >= 3) & (lane < 127), part, 3)
    for row in rows:
        middle, change = rate(second, row)
        begin = start[edge + row : edge + row + chunk]
        last = begin * (1.0 / 3.0) + (2.0 / 3.0) * (middle + time_step * change)
        other = jnp.where(component == 2, roll(last, 2 * STRIDE, 1), roll(last, -STRIDE, 1))
        fields = jnp.where(part == 0, last, 0.0)
        fields = jnp.where(part == 1, roll(last * last, 4, 1), fields)
        first[row : row + chunk] = jnp.where(part == 2, roll(last * other, 8, 1), fields)
        sorted_cells = picked(jnp.where(part == 0, last, 0.0), sort_cells[...])
        start[edge + row : edge + row + chunk] = sorted_cells[:, :LANES]
        rest = jnp.where(lane // 16 == in_eight, sorted_cells[:, LANES:], 0.0)
        rest = jnp.sum(rest.reshape(chunk // 8, 8, LANES), axis=1)
        for block in range(chunk // 16):
            place = (row // 16 + block) * BACK + 16
            out[place : place + 2] = rest[2 * block : 2 * block + 2]
    coeffs = picked(table_dot(table[0], table[1], first[:NZ]), sort_fields[...]) * mask[...]
    filtered = table_dot(synth[0], synth[1], coeffs) + start[edge : edge + NZ]
    for block in range(GZ):
        out[block * BACK : block * BACK + 16] = filtered[16 * block : 16 * block + 16]


def forward_body(cells, out):
    for row in range(TILE_Z):
        out[row] = cells[pl.ds(row, GZ, stride=BACK), :]


def unsort():
    source = lax.broadcasted_iota(jnp.int32, (LANES, LANES), 0)
    target = lax.broadcasted_iota(jnp.int32, (LANES, LANES), 1)
    return jnp.where(target == source % 32 * 4 + source // 32, 1.0, 0.0).astype(jnp.bfloat16)


def cells_body(cells, out, rows):
    lane = lanes_of(8)
    rest = jnp.concatenate(
        [cells[pl.ds(16 + half, GZ, stride=BACK), :] for half in range(2)] * 2, axis=0
    ).T
    for group in range(4):
        turned = jnp.concatenate(
            [cells[pl.ds(4 * group + r, GZ, stride=BACK), :] for r in range(4)], axis=0
        ).T
        for r in range(4):
            row = 4 * group + r
            for begin, source, count, at in (
                (4 * FIELDS, turned, 5, r),
                (row % 8 * 16, rest, 4, row // 8),
            ):
                joined = jnp.zeros((count, LANES), jnp.float32)
                for column in range(4):
                    low = begin + column * count
                    moved = roll(source[low : low + count], (column - at) * 32, 1)
                    joined = jnp.where(lane[:count] // 32 == column, moved, joined)
                place = row * 16 + (0 if count == 5 else 5)
                rows[place : place + count] = joined
            rows[row * 16 + 9 : row * 16 + 16] = jnp.zeros((7, LANES), jnp.float32)
    order = unsort()
    rows[...] = picked(rows[...], order)
    for c in range(3):
        for p in range(PLANES):
            out[c, p] = rows[pl.ds(c * PLANES + p, TILE_Z, stride=16), :]


def streamwise_body(lines, mask, table, out, rows):
    cells = lines[...].reshape(NX // 4, LANES)
    coeffs = table_dot(table[0, 0], table[0, 1], cells)
    for column in range(1, 4):
        coeffs = coeffs + roll(
            table_dot(table[column, 0], table[column, 1], cells), -FIELDS * column, 1
        )
    coeffs = jnp.where(lanes_of(MODES) < FIELDS, coeffs * mask[...], 0.0).T[:32]
    rows[...] = jnp.zeros(rows.shape, jnp.float32)
    for column in range(4):
        filtered = dot_table(coeffs, table[column, 0], table[column, 1])
        for q, (a, b) in enumerate(zip(pair_first, pair_second)):
            rows[column, 3 * q : 3 * q + 3] = (
                filtered[9 + 3 * q : 12 + 3 * q]
                - filtered[3 * a : 3 * a + 3] * filtered[3 * b : 3 * b + 3]
            )
    lane = lanes_of(24)
    for dest in range(GX):
        begin = dest // 4 * LANES
        joined = jnp.zeros((24, LANES), jnp.float32)
        for column in range(4):
            moved = roll(rows[column, :, begin : begin + LANES], (column - dest % 4) * 32, 1)
            joined = jnp.where(lane // 32 == column, moved, joined)
        out[dest * STRESSES : (dest + 1) * STRESSES] = joined[:STRESSES]


def stress_body(lines, out, rows):
    rows[...] = picked(lines[...], unsort())
    for q in range(6):
        for p in range(PLANES):
            out[q, p] = rows[pl.ds(q * PLANES + p, TILE_Z, stride=STRESSES), :]


def wave_table(length):
    column = np.arange(MODES)
    numbers = np.where(column < HALF, column, column - HALF + 1)
    angles = (np.arange(length)[:, None] * numbers[None, :] % length) * (2.0 * math.pi / length)
    return np.where(column[None, :] < HALF, np.cos(angles), np.sin(angles))


def wave_tables():
    synth_z = wave_table(NZ).T
    synth_x = wave_table(NX).reshape(NX // 4, 4, MODES).transpose(1, 2, 0)
    sort_fields = np.zeros((LANES, LANES))
    sort_cells = np.zeros((LANES, 2 * LANES))
    kinds = ((0, 1, 2), (3, 6, 8), (4, 7, 5))
    for c in range(3):
        for p in range(PLANES):
            for column in range(4):
                lane = c * STRIDE + p * SLOT + 3 + column
                for kind in range(3):
                    field = kinds[kind][c] * PLANES + p
                    sort_fields[lane + 4 * kind, column * FIELDS + field] = 1.0
                index = c * PLANES + p
                if index < 5:
                    sort_cells[lane, 4 * FIELDS + column * 5 + index] = 1.0
                else:
                    begin = LANES + column * 4 + index - 5
                    sort_cells[lane, begin : 2 * LANES : 16] = 1.0

    def halves(values):
        high = values.astype(jnp.bfloat16)
        low = (values - high.astype(np.float64)).astype(jnp.bfloat16)
        return np.stack([high, low], axis=-3)

    return [
        jnp.asarray(np.ascontiguousarray(values))
        for values in (
            halves(synth_z),
            halves(synth_z.T),
            sort_fields.astype(jnp.bfloat16),
            sort_cells.astype(jnp.bfloat16),
            halves(synth_x),
        )
    ]


def exchange(rows, axis, count):
    sent = rows.reshape(count, -1, 2, LANES)
    return lax.all_to_all(sent, axis, 0, 0, tiled=True).reshape(rows.shape)


def local(velocity, downflow, shear, mode_counts):
    count = lax.axis_size("gx")
    mode_counts = mode_counts.T
    left = lax.ppermute(velocity, "gx", [(i, (i + 1) % count) for i in range(count)])
    right = lax.ppermute(velocity, "gx", [((i + 1) % count, i) for i in range(count)])
    tables = [velocity, *wave_tables()]
    inner, flow, slope, mask_z, mask_x, *tables = call(
        inner_body,
        [(GZ, TILE_Z, LANES), (8, LANES), (8, LANES), (MODES, LANES), (MODES, LANES), *tables],
        3,
        [],
        downflow,
        shear,
        mode_counts,
        *tables,
        tables=6,
    )
    own, analysis_z, synth_z, sort_fields, sort_cells, synth_x = tables
    (cells,) = call(
        outer_body,
        [(GZ, TILE_Z, LANES)],
        0,
        [],
        own,
        left,
        right,
        inner,
        alias={3: 0},
    )
    cells = lax.all_to_all(cells, spanwise, 0, 0, tiled=True)
    (cells,) = call(
        advance_body,
        [(GZ * BACK, LANES)],
        0,
        [(NZ + 16, LANES)] * 3,
        cells,
        flow,
        slope,
        mask_z,
        analysis_z,
        synth_z,
        sort_fields,
        sort_cells,
    )
    cells = exchange(cells, spanwise, GZ)
    (lines,) = call(forward_body, [(GX, GZ, LANES)], 0, [], cells)
    lines = lax.all_to_all(lines, "gx", 0, 0, tiled=True)
    (advanced,) = call(
        cells_body, [(3, PLANES, TILE_Z, TILE_X)], 0, [(16 * TILE_Z, LANES)], cells, final=True
    )
    (lines,) = call(
        streamwise_body,
        [(GX * STRESSES, LANES)],
        0,
        [(4, 24, NX // 4)],
        lines,
        mask_x,
        synth_x,
    )
    lines = exchange(lines, "gx", GX)
    (stress,) = call(
        stress_body, [(6, PLANES, TILE_Z, TILE_X)], 0, [(GX * STRESSES, LANES)], lines, final=True
    )
    return advanced, stress


def solution(mesh):
    return jax.shard_map(
        local,
        mesh=mesh,
        in_specs=(P(None, None, ("gz", "grp"), "gx"), P(), P(), P()),
        out_specs=(P(None, None, ("gz", "grp"), "gx"), P(None, None, ("gz", "grp"), "gx")),
        check_vma=False,
    )
```

```python
import math

import jax
import jax.numpy as jnp
import numpy as np
from jax import lax
from jax.experimental import pallas as pl
from jax.experimental.pallas import tpu as pltpu
from jax.sharding import PartitionSpec as P

NX = 2048
NZ = 512
MODES = 256
HALF = MODES // 2
PLANES = 3
TILE_Z = 16
TILE_X = 128
GX = NX // TILE_X
GZ = NZ // TILE_Z
LANES = 128

SLOT = 14
STRIDE = PLANES * SLOT
FIELDS = 9 * PLANES
BACK = 18
SENT = 12
STRESSES = 6 * PLANES

molecular_diffusivity = 0.4
time_step = 0.2
spanwise = ("gz", "grp")
pair_first = (0, 0, 0, 1, 1, 2)
pair_second = (0, 1, 2, 1, 2, 2)


def roll(values, shift, axis):
    shift = shift % values.shape[axis]
    return pltpu.roll(values, shift, axis) if shift else values


def call(body, out_shapes, smem, scratch, *args, tables=0, final=False, alias=None):
    make = jax.ShapeDtypeStruct if final else pltpu.VMEM
    near = len(args) - tables
    args = (
        tuple(pltpu.with_memory_space_constraint(arg, pltpu.HBM) for arg in args[:smem])
        + tuple(pltpu.with_memory_space_constraint(arg, pltpu.VMEM) for arg in args[smem:near])
        + tuple(pltpu.with_memory_space_constraint(arg, pltpu.HBM) for arg in args[near:])
    )
    return pl.pallas_call(
        body,
        out_shape=[
            make(shape.shape, shape.dtype)
            if isinstance(shape, jax.Array)
            else make(shape, jnp.float32)
            for shape in out_shapes
        ],
        in_specs=[pl.BlockSpec(memory_space=pltpu.SMEM)] * smem
        + [pl.BlockSpec(memory_space=pltpu.VMEM)] * (near - smem)
        + [pl.BlockSpec(memory_space=pltpu.HBM)] * tables,
        out_specs=[pl.BlockSpec(memory_space=pltpu.VMEM)] * len(out_shapes),
        scratch_shapes=[pltpu.VMEM(shape, jnp.float32) for shape in scratch]
        + ([pltpu.SemaphoreType.DMA((tables,))] if tables else []),
        compiler_params=pltpu.CompilerParams(vmem_limit_bytes=16 << 20),
        input_output_aliases=alias or {},
    )(*args)


def dot(left, right):
    return lax.dot_general(
        left,
        right,
        (((1,), (0,)), ((), ())),
        precision=lax.Precision.DEFAULT,
        preferred_element_type=jnp.float32,
    )


def parts(values, count):
    terms = []
    for index in range(count):
        terms.append(values.astype(jnp.bfloat16))
        if index + 1 < count:
            values = values - terms[-1].astype(jnp.float32)
    return terms


def picked(values, choice):
    rows = values.shape[0]
    sums = dot(jnp.concatenate(parts(values, 3), axis=0), choice)
    return sums[:rows] + (sums[rows : 2 * rows] + sums[2 * rows :])


def table_dot(high, low, values):
    width = values.shape[1]
    large, small = parts(values, 2)
    sums = dot(high, jnp.concatenate([large, small], axis=1))
    return sums[:, :width] + (sums[:, width:] + dot(low, large))


def dot_table(values, high, low):
    rows = values.shape[0]
    large, small = parts(values, 2)
    sums = dot(jnp.concatenate([large, small], axis=0), high)
    return sums[:rows] + (sums[rows:] + dot(large, low))


def lanes_of(rows):
    return lax.broadcasted_iota(jnp.int32, (rows, LANES), 1)


def pack_for(out, dest, sides):
    lane = lanes_of(TILE_Z)
    packed = jnp.zeros((TILE_Z, LANES), jnp.float32)
    for index, values in enumerate(sides):
        moved = roll(values, index * SLOT - (4 * dest - 3), 1)
        here = (lane >= index * SLOT) & (lane < index * SLOT + 10)
        packed = jnp.where(here, moved, packed)
    own_lane = lanes_of(4) % SLOT < 10
    for part in range(3):
        rest = roll(packed[SENT:], 10 - 4 * part, 1)
        place = dest * SENT + 4 * part
        out[place : place + 4] = jnp.where(own_lane, packed[4 * part : 4 * part + 4], rest)


def inner_body(downflow, shear, counts, *refs):
    far = refs[:6]
    out, flow, slope, mask_z, mask_x = refs[6:11]
    near = refs[11:17]
    done = refs[17]
    fetches = [
        pltpu.make_async_copy(source, target, done.at[index])
        for index, (source, target) in enumerate(zip(far, near))
    ]
    for fetch in fetches:
        fetch.start()
    fetches[0].wait()
    cells = [near[0][c, p] for c in range(3) for p in range(PLANES)]
    for dest in range(1, GZ - 1):
        pack_for(out, dest, cells)
    lane = lanes_of(8)
    plane = lane % STRIDE // SLOT
    speeds = jnp.zeros((8, LANES), jnp.float32)
    shears = jnp.zeros((8, LANES), jnp.float32)
    for p in range(PLANES):
        speeds = jnp.where(plane == p, downflow[p], speeds)
        shears = jnp.where((plane == p) & (lane < STRIDE), shear[p], shears)
    flow[...] = speeds
    slope[...] = shears
    mode = lax.broadcasted_iota(jnp.int32, (MODES, LANES), 0)
    number = jnp.where(mode < HALF, mode, mode - HALF + 1)
    plane = lanes_of(MODES) % PLANES
    for mask, axis, length in ((mask_z, 1, NZ), (mask_x, 0, NX)):
        limit = jnp.zeros((MODES, LANES), jnp.int32)
        for p in range(PLANES):
            limit = jnp.where(plane == p, counts[axis, p], limit)
        weight = jnp.where(mode == 0, 1.0 / length, 2.0 / length)
        mask[...] = jnp.where(number <= limit, weight, 0.0)
    for fetch in fetches[1:]:
        fetch.wait()


def outer_body(own, left, right, inner, out):
    low = lanes_of(TILE_Z) < LANES // 2
    pairs = [(c, p) for c in range(3) for p in range(PLANES)]
    pack_for(out, 0, [jnp.where(low, own[c, p], left[c, p]) for c, p in pairs])
    pack_for(out, GZ - 1, [jnp.where(low, right[c, p], own[c, p]) for c, p in pairs])


def advance_body(
    cells, flow_row, slope_row, mask, table, synth, sort_fields, sort_cells,
    out, start, first, second,
):
    chunk = 64
    edge = 8
    lane = lanes_of(chunk)
    component = lane // STRIDE
    flow = jnp.broadcast_to(flow_row[:1], (chunk, LANES))
    slope = jnp.broadcast_to(slope_row[:1], (chunk, LANES))

    def store(ref, row, values):
        ref[edge + row : edge + row + chunk] = values
        if row == 0:
            ref[edge + NZ : edge + NZ + edge] = values[:edge]
        if row == NZ - chunk:
            ref[:edge] = values[chunk - edge :]

    def rate(ref, row):
        low = edge + row
        middle = ref[low : low + chunk]
        north = ref[low + 1 : low + 1 + chunk]
        south = ref[low - 1 : low - 1 + chunk]
        east = roll(middle, -1, 1)
        west = roll(middle, 1, 1)
        next_one = roll(middle, -STRIDE, 1)
        along = jnp.where(
            component == 0,
            middle,
            jnp.where(component == 1, roll(middle, STRIDE, 1), roll(middle, 2 * STRIDE, 1)),
        )
        across = jnp.where(
            component == 2,
            middle,
            jnp.where(component == 1, next_one, roll(middle, -2 * STRIDE, 1)),
        )
        return middle, (
            -(flow + along) * ((east - west) * 0.5)
            - across * ((north - south) * 0.5)
            + molecular_diffusivity * (east + west + north + south - 4.0 * middle)
            - slope * next_one
        )

    rows = range(0, NZ, chunk)
    column = lanes_of(4) % SLOT
    for block in range(GZ):
        rest = jnp.zeros((4, LANES), jnp.float32)
        place = edge + block * 16
        for index in range(3):
            piece = cells[block * SENT + 4 * index : block * SENT + 4 * index + 4]
            start[place + 4 * index : place + 4 * index + 4] = piece
            rest = jnp.where(column // 4 == index, roll(piece, 4 * index - 10, 1), rest)
        start[place + SENT : place + 16] = rest
    start[:edge] = start[NZ : NZ + edge]
    start[edge + NZ :] = start[edge : 2 * edge]
    for row in rows:
        middle, change = rate(start, row)
        store(first, row, middle + time_step * change)
    for row in rows:
        middle, change = rate(first, row)
        begin = start[edge + row : edge + row + chunk]
        store(second, row, 0.75 * begin + 0.25 * (middle + time_step * change))
    in_eight = lax.broadcasted_iota(jnp.int32, (chunk, LANES), 0) % 8
    part = (lane + LANES - 3) % LANES % SLOT // 4
    part = jnp.where((lane >= 3) & (lane < 127), part, 3)
    for row in rows:
        middle, change = rate(second, row)
        begin = start[edge + row : edge + row + chunk]
        last = begin * (1.0 / 3.0) + (2.0 / 3.0) * (middle + time_step * change)
        other = jnp.where(component == 2, roll(last, 2 * STRIDE, 1), roll(last, -STRIDE, 1))
        fields = jnp.where(part == 0, last, 0.0)
        fields = jnp.where(part == 1, roll(last * last, 4, 1), fields)
        first[row : row + chunk] = jnp.where(part == 2, roll(last * other, 8, 1), fields)
        sorted_cells = picked(jnp.where(part == 0, last, 0.0), sort_cells[...])
        start[edge + row : edge + row + chunk] = sorted_cells[:, :LANES]
        rest = jnp.where(lane // 16 == in_eight, sorted_cells[:, LANES:], 0.0)
        rest = jnp.sum(rest.reshape(chunk // 8, 8, LANES), axis=1)
        for block in range(chunk // 16):
            place = (row // 16 + block) * BACK + 16
            out[place : place + 2] = rest[2 * block : 2 * block + 2]
    coeffs = picked(table_dot(table[0], table[1], first[:NZ]), sort_fields[...]) * mask[...]
    filtered = table_dot(synth[0], synth[1], coeffs) + start[edge : edge + NZ]
    for block in range(GZ):
        out[block * BACK : block * BACK + 16] = filtered[16 * block : 16 * block + 16]


def forward_body(cells, out):
    for row in range(TILE_Z):
        out[row] = cells[pl.ds(row, GZ, stride=BACK), :]


def unsort():
    source = lax.broadcasted_iota(jnp.int32, (LANES, LANES), 0)
    target = lax.broadcasted_iota(jnp.int32, (LANES, LANES), 1)
    return jnp.where(target == source % 32 * 4 + source // 32, 1.0, 0.0).astype(jnp.bfloat16)


def cells_body(cells, out, rows):
    lane = lanes_of(8)
    rest = jnp.concatenate(
        [cells[pl.ds(16 + half, GZ, stride=BACK), :] for half in range(2)] * 2, axis=0
    ).T
    for group in range(4):
        turned = jnp.concatenate(
            [cells[pl.ds(4 * group + r, GZ, stride=BACK), :] for r in range(4)], axis=0
        ).T
        for r in range(4):
            row = 4 * group + r
            for begin, source, count, at in (
                (4 * FIELDS, turned, 5, r),
                (row % 8 * 16, rest, 4, row // 8),
            ):
                joined = jnp.zeros((count, LANES), jnp.float32)
                for column in range(4):
                    low = begin + column * count
                    moved = roll(source[low : low + count], (column - at) * 32, 1)
                    joined = jnp.where(lane[:count] // 32 == column, moved, joined)
                place = row * 16 + (0 if count == 5 else 5)
                rows[place : place + count] = joined
            rows[row * 16 + 9 : row * 16 + 16] = jnp.zeros((7, LANES), jnp.float32)
    order = unsort()
    rows[...] = picked(rows[...], order)
    for c in range(3):
        for p in range(PLANES):
            out[c, p] = rows[pl.ds(c * PLANES + p, TILE_Z, stride=16), :]


def streamwise_body(lines, mask, table, out, rows):
    cells = lines[...].reshape(NX // 4, LANES)
    coeffs = table_dot(table[0, 0], table[0, 1], cells)
    for column in range(1, 4):
        coeffs = coeffs + roll(
            table_dot(table[column, 0], table[column, 1], cells), -FIELDS * column, 1
        )
    coeffs = jnp.where(lanes_of(MODES) < FIELDS, coeffs * mask[...], 0.0).T[:32]
    rows[...] = jnp.zeros(rows.shape, jnp.float32)
    for column in range(4):
        filtered = dot_table(coeffs, table[column, 0], table[column, 1])
        for q, (a, b) in enumerate(zip(pair_first, pair_second)):
            rows[column, 3 * q : 3 * q + 3] = (
                filtered[9 + 3 * q : 12 + 3 * q]
                - filtered[3 * a : 3 * a + 3] * filtered[3 * b : 3 * b + 3]
            )
    lane = lanes_of(24)
    for dest in range(GX):
        begin = dest // 4 * LANES
        joined = jnp.zeros((24, LANES), jnp.float32)
        for column in range(4):
            moved = roll(rows[column, :, begin : begin + LANES], (column - dest % 4) * 32, 1)
            joined = jnp.where(lane // 32 == column, moved, joined)
        out[dest * STRESSES : (dest + 1) * STRESSES] = joined[:STRESSES]


def stress_body(lines, out, rows):
    rows[...] = picked(lines[...], unsort())
    for q in range(6):
        for p in range(PLANES):
            out[q, p] = rows[pl.ds(q * PLANES + p, TILE_Z, stride=STRESSES), :]


def wave_table(length):
    column = np.arange(MODES)
    numbers = np.where(column < HALF, column, column - HALF + 1)
    angles = (np.arange(length)[:, None] * numbers[None, :] % length) * (2.0 * math.pi / length)
    return np.where(column[None, :] < HALF, np.cos(angles), np.sin(angles))


def wave_tables():
    synth_z = wave_table(NZ).T
    synth_x = wave_table(NX).reshape(NX // 4, 4, MODES).transpose(1, 2, 0)
    sort_fields = np.zeros((LANES, LANES))
    sort_cells = np.zeros((LANES, 2 * LANES))
    kinds = ((0, 1, 2), (3, 6, 8), (4, 7, 5))
    for c in range(3):
        for p in range(PLANES):
            for column in range(4):
                lane = c * STRIDE + p * SLOT + 3 + column
                for kind in range(3):
                    field = kinds[kind][c] * PLANES + p
                    sort_fields[lane + 4 * kind, column * FIELDS + field] = 1.0
                index = c * PLANES + p
                if index < 5:
                    sort_cells[lane, 4 * FIELDS + column * 5 + index] = 1.0
                else:
                    begin = LANES + column * 4 + index - 5
                    sort_cells[lane, begin : 2 * LANES : 16] = 1.0

    def halves(values):
        high = values.astype(jnp.bfloat16)
        low = (values - high.astype(np.float64)).astype(jnp.bfloat16)
        return np.stack([high, low], axis=-3)

    return [
        jnp.asarray(np.ascontiguousarray(values))
        for values in (
            halves(synth_z),
            halves(synth_z.T),
            sort_fields.astype(jnp.bfloat16),
            sort_cells.astype(jnp.bfloat16),
            halves(synth_x),
        )
    ]


def exchange(rows, axis, count):
    sent = rows.reshape(count, -1, 2, LANES)
    return lax.all_to_all(sent, axis, 0, 0, tiled=True).reshape(rows.shape)


def local(velocity, downflow, shear, mode_counts):
    count = lax.axis_size("gx")
    mode_counts = mode_counts.T
    left = lax.ppermute(velocity, "gx", [(i, (i + 1) % count) for i in range(count)])
    right = lax.ppermute(velocity, "gx", [((i + 1) % count, i) for i in range(count)])
    tables = [velocity, *wave_tables()]
    inner, flow, slope, mask_z, mask_x, *tables = call(
        inner_body,
        [(GZ * SENT, LANES), (8, LANES), (8, LANES), (MODES, LANES), (MODES, LANES), *tables],
        3,
        [],
        downflow,
        shear,
        mode_counts,
        *tables,
        tables=6,
    )
    own, analysis_z, synth_z, sort_fields, sort_cells, synth_x = tables
    (cells,) = call(
        outer_body,
        [(GZ * SENT, LANES)],
        0,
        [],
        own,
        left,
        right,
        inner,
        alias={3: 0},
    )
    cells = exchange(cells, spanwise, GZ)
    (cells,) = call(
        advance_body,
        [(GZ * BACK, LANES)],
        0,
        [(NZ + 16, LANES)] * 3,
        cells,
        flow,
        slope,
        mask_z,
        analysis_z,
        synth_z,
        sort_fields,
        sort_cells,
    )
    cells = exchange(cells, spanwise, GZ)
    (lines,) = call(forward_body, [(GX, GZ, LANES)], 0, [], cells)
    lines = lax.all_to_all(lines, "gx", 0, 0, tiled=True)
    (advanced,) = call(
        cells_body, [(3, PLANES, TILE_Z, TILE_X)], 0, [(16 * TILE_Z, LANES)], cells, final=True
    )
    (lines,) = call(
        streamwise_body,
        [(GX * STRESSES, LANES)],
        0,
        [(4, 24, NX // 4)],
        lines,
        mask_x,
        synth_x,
    )
    lines = exchange(lines, "gx", GX)
    (stress,) = call(
        stress_body, [(6, PLANES, TILE_Z, TILE_X)], 0, [(GX * STRESSES, LANES)], lines, final=True
    )
    return advanced, stress


def solution(mesh):
    return jax.shard_map(
        local,
        mesh=mesh,
        in_specs=(P(None, None, ("gz", "grp"), "gx"), P(), P(), P()),
        out_specs=(P(None, None, ("gz", "grp"), "gx"), P(None, None, ("gz", "grp"), "gx")),
        check_vma=False,
    )
```

```python
import math

import jax
import jax.numpy as jnp
import numpy as np
from jax import lax
from jax.experimental import pallas as pl
from jax.experimental.pallas import tpu as pltpu
from jax.sharding import PartitionSpec as P

NX = 2048
NZ = 512
MODES = 256
HALF = MODES // 2
PLANES = 3
TILE_Z = 16
TILE_X = 128
GX = NX // TILE_X
GZ = NZ // TILE_Z
LANES = 128

SLOT = 14
STRIDE = PLANES * SLOT
FIELDS = 9 * PLANES
BACK = 18
SENT = 12
STRESSES = 6 * PLANES

molecular_diffusivity = 0.4
time_step = 0.2
spanwise = ("gz", "grp")
pair_first = (0, 0, 0, 1, 1, 2)
pair_second = (0, 1, 2, 1, 2, 2)


def roll(values, shift, axis):
    shift = shift % values.shape[axis]
    return pltpu.roll(values, shift, axis) if shift else values


def call(body, out_shapes, smem, scratch, *args, tables=0, final=False, alias=None, extra=()):
    make = jax.ShapeDtypeStruct if final else pltpu.VMEM
    near = len(args) - tables
    args = (
        tuple(pltpu.with_memory_space_constraint(arg, pltpu.HBM) for arg in args[:smem])
        + tuple(pltpu.with_memory_space_constraint(arg, pltpu.VMEM) for arg in args[smem:near])
        + tuple(pltpu.with_memory_space_constraint(arg, pltpu.HBM) for arg in args[near:])
    )
    return pl.pallas_call(
        body,
        out_shape=[
            make(shape.shape, shape.dtype)
            if isinstance(shape, jax.Array)
            else make(shape, jnp.float32)
            for shape in out_shapes
        ],
        in_specs=[pl.BlockSpec(memory_space=pltpu.SMEM)] * smem
        + [pl.BlockSpec(memory_space=pltpu.VMEM)] * (near - smem)
        + [pl.BlockSpec(memory_space=pltpu.HBM)] * tables,
        out_specs=[pl.BlockSpec(memory_space=pltpu.VMEM)] * len(out_shapes),
        scratch_shapes=[pltpu.VMEM(shape, jnp.float32) for shape in scratch]
        + list(extra)
        + ([pltpu.SemaphoreType.DMA((tables,))] if tables else []),
        compiler_params=pltpu.CompilerParams(vmem_limit_bytes=16 << 20),
        input_output_aliases=alias or {},
    )(*args)


def dot(left, right):
    return lax.dot_general(
        left,
        right,
        (((1,), (0,)), ((), ())),
        precision=lax.Precision.DEFAULT,
        preferred_element_type=jnp.float32,
    )


def parts(values, count):
    terms = []
    for index in range(count):
        terms.append(values.astype(jnp.bfloat16))
        if index + 1 < count:
            values = values - terms[-1].astype(jnp.float32)
    return terms


def picked(values, choice):
    rows = values.shape[0]
    sums = dot(jnp.concatenate(parts(values, 3), axis=0), choice)
    return sums[:rows] + (sums[rows : 2 * rows] + sums[2 * rows :])


def table_dot(high, low, values):
    width = values.shape[1]
    large, small = parts(values, 2)
    sums = dot(high, jnp.concatenate([large, small], axis=1))
    return sums[:, :width] + (sums[:, width:] + dot(low, large))


def dot_table(values, high, low):
    rows = values.shape[0]
    large, small = parts(values, 2)
    sums = dot(jnp.concatenate([large, small], axis=0), high)
    return sums[:rows] + (sums[rows:] + dot(large, low))


def lanes_of(rows):
    return lax.broadcasted_iota(jnp.int32, (rows, LANES), 1)


def pack_for(out, dest, sides):
    lane = lanes_of(TILE_Z)
    packed = jnp.zeros((TILE_Z, LANES), jnp.float32)
    for index, values in enumerate(sides):
        moved = roll(values, index * SLOT - (4 * dest - 3), 1)
        here = (lane >= index * SLOT) & (lane < index * SLOT + 10)
        packed = jnp.where(here, moved, packed)
    own_lane = lanes_of(8) % SLOT < 10
    low = lax.broadcasted_iota(jnp.int32, (8, LANES), 0) < 4
    last = packed[8:]
    turned = roll(last, 4, 0)
    rest = jnp.where(low, roll(turned, 10, 1), roll(last, 6, 1))
    place = dest * SENT
    out[place : place + 8] = jnp.where(own_lane, packed[:8], rest)
    out[place + 8 : place + SENT] = jnp.where(own_lane, last, roll(turned, 2, 1))[:4]


def inner_body(*refs):
    far = refs[:9]
    out, flow, slope, mask_z, mask_x = refs[9:14]
    near = refs[14:23]
    downflow, shear, counts = refs[20:23]
    done = refs[23]
    fetches = [
        pltpu.make_async_copy(source, target, done.at[index])
        for index, (source, target) in enumerate(zip(far, near))
    ]
    for fetch in fetches:
        fetch.start()
    fetches[0].wait()
    cells = [near[0][c, p] for c in range(3) for p in range(PLANES)]
    for dest in range(1, GZ - 1):
        pack_for(out, dest, cells)
    for fetch in fetches[6:]:
        fetch.wait()
    lane = lanes_of(8)
    plane = lane % STRIDE // SLOT
    speeds = jnp.zeros((8, LANES), jnp.float32)
    shears = jnp.zeros((8, LANES), jnp.float32)
    for p in range(PLANES):
        speeds = jnp.where(plane == p, downflow[p], speeds)
        shears = jnp.where((plane == p) & (lane < STRIDE), shear[p], shears)
    flow[...] = speeds
    slope[...] = shears
    mode = lax.broadcasted_iota(jnp.int32, (MODES, LANES), 0)
    number = jnp.where(mode < HALF, mode, mode - HALF + 1)
    plane = lanes_of(MODES) % PLANES
    for mask, axis, length in ((mask_z, 1, NZ), (mask_x, 0, NX)):
        limit = jnp.zeros((MODES, LANES), jnp.int32)
        for p in range(PLANES):
            limit = jnp.where(plane == p, counts[axis, p], limit)
        weight = jnp.where(mode == 0, 1.0 / length, 2.0 / length)
        mask[...] = jnp.where(number <= limit, weight, 0.0)
    for fetch in fetches[1:6]:
        fetch.wait()


def outer_body(own, left, right, inner, out):
    low = lanes_of(TILE_Z) < LANES // 2
    pairs = [(c, p) for c in range(3) for p in range(PLANES)]
    pack_for(out, 0, [jnp.where(low, own[c, p], left[c, p]) for c, p in pairs])
    pack_for(out, GZ - 1, [jnp.where(low, right[c, p], own[c, p]) for c, p in pairs])


def advance_body(
    cells, flow_row, slope_row, mask, table, synth, sort_fields, sort_cells,
    out, start, first, second,
):
    chunk = 64
    edge = 8
    lane = lanes_of(chunk)
    component = lane // STRIDE
    flow = jnp.broadcast_to(flow_row[:1], (chunk, LANES))
    slope = jnp.broadcast_to(slope_row[:1], (chunk, LANES))

    def store(ref, row, values):
        ref[edge + row : edge + row + chunk] = values
        if row == 0:
            ref[edge + NZ : edge + NZ + edge] = values[:edge]
        if row == NZ - chunk:
            ref[:edge] = values[chunk - edge :]

    def rate(ref, row):
        low = edge + row
        middle = ref[low : low + chunk]
        north = ref[low + 1 : low + 1 + chunk]
        south = ref[low - 1 : low - 1 + chunk]
        east = roll(middle, -1, 1)
        west = roll(middle, 1, 1)
        next_one = roll(middle, -STRIDE, 1)
        along = jnp.where(
            component == 0,
            middle,
            jnp.where(component == 1, roll(middle, STRIDE, 1), roll(middle, 2 * STRIDE, 1)),
        )
        across = jnp.where(
            component == 2,
            middle,
            jnp.where(component == 1, next_one, roll(middle, -2 * STRIDE, 1)),
        )
        return middle, (
            -(flow + along) * ((east - west) * 0.5)
            - across * ((north - south) * 0.5)
            + molecular_diffusivity * (east + west + north + south - 4.0 * middle)
            - slope * next_one
        )

    rows = range(0, NZ, chunk)
    column = lanes_of(4) % SLOT
    for block in range(GZ):
        rest = jnp.zeros((4, LANES), jnp.float32)
        place = edge + block * 16
        for index in range(3):
            piece = cells[block * SENT + 4 * index : block * SENT + 4 * index + 4]
            start[place + 4 * index : place + 4 * index + 4] = piece
            rest = jnp.where(column // 4 == index, roll(piece, 4 * index - 10, 1), rest)
        start[place + SENT : place + 16] = rest
    start[:edge] = start[NZ : NZ + edge]
    start[edge + NZ :] = start[edge : 2 * edge]
    for row in rows:
        middle, change = rate(start, row)
        store(first, row, middle + time_step * change)
    for row in rows:
        middle, change = rate(first, row)
        begin = start[edge + row : edge + row + chunk]
        store(second, row, 0.75 * begin + 0.25 * (middle + time_step * change))
    part = (lane + LANES - 3) % LANES % SLOT // 4
    part = jnp.where((lane >= 3) & (lane < 127), part, 3)
    for row in rows:
        middle, change = rate(second, row)
        begin = start[edge + row : edge + row + chunk]
        last = begin * (1.0 / 3.0) + (2.0 / 3.0) * (middle + time_step * change)
        other = jnp.where(component == 2, roll(last, 2 * STRIDE, 1), roll(last, -STRIDE, 1))
        fields = jnp.where(part == 0, last, 0.0)
        fields = jnp.where(part == 1, roll(last * last, 4, 1), fields)
        first[row : row + chunk] = jnp.where(part == 2, roll(last * other, 8, 1), fields)
        sorted_cells = picked(jnp.where(part == 0, last, 0.0), sort_cells[...])
        start[edge + row : edge + row + chunk] = jnp.where(lane < 16, 0.0, sorted_cells)
        rest = jnp.where(lane < 16, sorted_cells, 0.0)
        rest = pltpu.roll(rest, 0, 1, stride=16, stride_axis=0)
        rest = jnp.sum(rest.reshape(chunk // 8, 8, LANES), axis=1)
        for block in range(chunk // 16):
            place = (row // 16 + block) * BACK + 16
            out[place : place + 2] = rest[2 * block : 2 * block + 2]
    coeffs = picked(table_dot(table[0], table[1], first[:NZ]), sort_fields[...]) * mask[...]
    filtered = table_dot(synth[0], synth[1], coeffs) + start[edge : edge + NZ]
    for block in range(GZ):
        out[block * BACK : block * BACK + 16] = filtered[16 * block : 16 * block + 16]


def forward_body(cells, out):
    for row in range(TILE_Z):
        out[row] = cells[pl.ds(row, GZ, stride=BACK), :]


def unsort():
    source = lax.broadcasted_iota(jnp.int32, (LANES, LANES), 0)
    target = lax.broadcasted_iota(jnp.int32, (LANES, LANES), 1)
    return jnp.where(target == source % 32 * 4 + source // 32, 1.0, 0.0).astype(jnp.bfloat16)


def cells_body(cells, out, rows):
    lane = lanes_of(8)
    rest = jnp.concatenate(
        [cells[pl.ds(16 + half, GZ, stride=BACK), :] for half in range(2)] * 2, axis=0
    ).T
    for group in range(4):
        turned = jnp.concatenate(
            [cells[pl.ds(4 * group + r, GZ, stride=BACK), :] for r in range(4)], axis=0
        ).T
        for r in range(4):
            row = 4 * group + r
            for begin, source, count, at in (
                (4 * FIELDS, turned, 5, r),
                (row % 8 * 16, rest, 4, row // 8),
            ):
                joined = jnp.zeros((count, LANES), jnp.float32)
                for column in range(4):
                    low = begin + column * count
                    moved = roll(source[low : low + count], (column - at) * 32, 1)
                    joined = jnp.where(lane[:count] // 32 == column, moved, joined)
                place = row * 16 + (0 if count == 5 else 5)
                rows[place : place + count] = joined
            rows[row * 16 + 9 : row * 16 + 16] = jnp.zeros((7, LANES), jnp.float32)
    order = unsort()
    rows[...] = picked(rows[...], order)
    for c in range(3):
        for p in range(PLANES):
            out[c, p] = rows[pl.ds(c * PLANES + p, TILE_Z, stride=16), :]


def streamwise_body(lines, mask, table, out, rows):
    cells = lines[...].reshape(NX // 4, LANES)
    coeffs = table_dot(table[0, 0], table[0, 1], cells)
    for column in range(1, 4):
        coeffs = coeffs + roll(
            table_dot(table[column, 0], table[column, 1], cells), -FIELDS * column, 1
        )
    coeffs = jnp.where(lanes_of(MODES) < FIELDS, coeffs * mask[...], 0.0).T[:32]
    rows[...] = jnp.zeros(rows.shape, jnp.float32)
    for column in range(4):
        filtered = dot_table(coeffs, table[column, 0], table[column, 1])
        for q, (a, b) in enumerate(zip(pair_first, pair_second)):
            rows[column, 3 * q : 3 * q + 3] = (
                filtered[9 + 3 * q : 12 + 3 * q]
                - filtered[3 * a : 3 * a + 3] * filtered[3 * b : 3 * b + 3]
            )
    lane = lanes_of(24)
    for dest in range(GX):
        begin = dest // 4 * LANES
        joined = jnp.zeros((24, LANES), jnp.float32)
        for column in range(4):
            moved = roll(rows[column, :, begin : begin + LANES], (column - dest % 4) * 32, 1)
            joined = jnp.where(lane // 32 == column, moved, joined)
        out[dest * STRESSES : (dest + 1) * STRESSES] = joined[:STRESSES]


def stress_body(lines, out, rows):
    rows[...] = picked(lines[...], unsort())
    for q in range(6):
        for p in range(PLANES):
            out[q, p] = rows[pl.ds(q * PLANES + p, TILE_Z, stride=STRESSES), :]


def wave_table(length):
    column = np.arange(MODES)
    numbers = np.where(column < HALF, column, column - HALF + 1)
    angles = (np.arange(length)[:, None] * numbers[None, :] % length) * (2.0 * math.pi / length)
    return np.where(column[None, :] < HALF, np.cos(angles), np.sin(angles))


def wave_tables():
    synth_z = wave_table(NZ).T
    synth_x = wave_table(NX).reshape(NX // 4, 4, MODES).transpose(1, 2, 0)
    sort_fields = np.zeros((LANES, LANES))
    sort_cells = np.zeros((LANES, LANES))
    kinds = ((0, 1, 2), (3, 6, 8), (4, 7, 5))
    for c in range(3):
        for p in range(PLANES):
            for column in range(4):
                lane = c * STRIDE + p * SLOT + 3 + column
                for kind in range(3):
                    field = kinds[kind][c] * PLANES + p
                    sort_fields[lane + 4 * kind, column * FIELDS + field] = 1.0
                index = c * PLANES + p
                if index < 5:
                    sort_cells[lane, 4 * FIELDS + column * 5 + index] = 1.0
                else:
                    sort_cells[lane, column * 4 + index - 5] = 1.0

    def halves(values):
        high = values.astype(jnp.bfloat16)
        low = (values - high.astype(np.float64)).astype(jnp.bfloat16)
        return np.stack([high, low], axis=-3)

    return [
        jnp.asarray(np.ascontiguousarray(values))
        for values in (
            halves(synth_z),
            halves(synth_z.T),
            sort_fields.astype(jnp.bfloat16),
            sort_cells.astype(jnp.bfloat16),
            halves(synth_x),
        )
    ]


def exchange(rows, axis, count):
    sent = rows.reshape(count, -1, 2, LANES)
    return lax.all_to_all(sent, axis, 0, 0, tiled=True).reshape(rows.shape)


def local(velocity, downflow, shear, mode_counts):
    count = lax.axis_size("gx")
    mode_counts = mode_counts.T
    left = lax.ppermute(velocity, "gx", [(i, (i + 1) % count) for i in range(count)])
    right = lax.ppermute(velocity, "gx", [((i + 1) % count, i) for i in range(count)])
    tables = [velocity, *wave_tables()]
    inner, flow, slope, mask_z, mask_x, *tables = call(
        inner_body,
        [(GZ * SENT, LANES), (8, LANES), (8, LANES), (MODES, LANES), (MODES, LANES), *tables],
        0,
        [],
        *tables,
        downflow,
        shear,
        mode_counts,
        tables=9,
        extra=[
            pltpu.SMEM((PLANES,), jnp.float32),
            pltpu.SMEM((PLANES,), jnp.float32),
            pltpu.SMEM((2, PLANES), jnp.int32),
        ],
    )
    own, analysis_z, synth_z, sort_fields, sort_cells, synth_x = tables
    (cells,) = call(
        outer_body,
        [(GZ * SENT, LANES)],
        0,
        [],
        own,
        left,
        right,
        inner,
        alias={3: 0},
    )
    cells = exchange(cells, spanwise, GZ)
    (cells,) = call(
        advance_body,
        [(GZ * BACK, LANES)],
        0,
        [(NZ + 16, LANES)] * 3,
        cells,
        flow,
        slope,
        mask_z,
        analysis_z,
        synth_z,
        sort_fields,
        sort_cells,
    )
    cells = exchange(cells, spanwise, GZ)
    (lines,) = call(forward_body, [(GX, GZ, LANES)], 0, [], cells)
    lines = lax.all_to_all(lines, "gx", 0, 0, tiled=True)
    (advanced,) = call(
        cells_body, [(3, PLANES, TILE_Z, TILE_X)], 0, [(16 * TILE_Z, LANES)], cells, final=True
    )
    (lines,) = call(
        streamwise_body,
        [(GX * STRESSES, LANES)],
        0,
        [(4, 24, NX // 4)],
        lines,
        mask_x,
        synth_x,
    )
    lines = exchange(lines, "gx", GX)
    (stress,) = call(
        stress_body, [(6, PLANES, TILE_Z, TILE_X)], 0, [(GX * STRESSES, LANES)], lines, final=True
    )
    return advanced, stress


def solution(mesh):
    return jax.shard_map(
        local,
        mesh=mesh,
        in_specs=(P(None, None, ("gz", "grp"), "gx"), P(), P(), P()),
        out_specs=(P(None, None, ("gz", "grp"), "gx"), P(None, None, ("gz", "grp"), "gx")),
        check_vma=False,
    )
```

```python
import math

import jax
import jax.numpy as jnp
import numpy as np
from jax import lax
from jax.experimental import pallas as pl
from jax.experimental.pallas import tpu as pltpu
from jax.sharding import PartitionSpec as P

NX = 2048
NZ = 512
MODES = 256
HALF = MODES // 2
PLANES = 3
TILE_Z = 16
TILE_X = 128
GX = NX // TILE_X
GZ = NZ // TILE_Z
LANES = 128

SLOT = 14
STRIDE = PLANES * SLOT
FIELDS = 9 * PLANES
BACK = 18
SENT = 12
STRESSES = 6 * PLANES

molecular_diffusivity = 0.4
time_step = 0.2
spanwise = ("gz", "grp")
pair_first = (0, 0, 0, 1, 1, 2)
pair_second = (0, 1, 2, 1, 2, 2)


def roll(values, shift, axis):
    shift = shift % values.shape[axis]
    return pltpu.roll(values, shift, axis) if shift else values


def call(body, out_shapes, smem, scratch, *args, tables=0, final=False, alias=None, extra=()):
    make = jax.ShapeDtypeStruct if final else pltpu.VMEM
    near = len(args) - tables
    args = (
        tuple(pltpu.with_memory_space_constraint(arg, pltpu.HBM) for arg in args[:smem])
        + tuple(pltpu.with_memory_space_constraint(arg, pltpu.VMEM) for arg in args[smem:near])
        + tuple(pltpu.with_memory_space_constraint(arg, pltpu.HBM) for arg in args[near:])
    )
    return pl.pallas_call(
        body,
        out_shape=[
            make(shape.shape, shape.dtype)
            if isinstance(shape, jax.Array)
            else make(shape, jnp.float32)
            for shape in out_shapes
        ],
        in_specs=[pl.BlockSpec(memory_space=pltpu.SMEM)] * smem
        + [pl.BlockSpec(memory_space=pltpu.VMEM)] * (near - smem)
        + [pl.BlockSpec(memory_space=pltpu.HBM)] * tables,
        out_specs=[pl.BlockSpec(memory_space=pltpu.VMEM)] * len(out_shapes),
        scratch_shapes=[pltpu.VMEM(shape, jnp.float32) for shape in scratch]
        + list(extra)
        + ([pltpu.SemaphoreType.DMA((tables,))] if tables else []),
        compiler_params=pltpu.CompilerParams(vmem_limit_bytes=16 << 20),
        input_output_aliases=alias or {},
    )(*args)


def dot(left, right):
    return lax.dot_general(
        left,
        right,
        (((1,), (0,)), ((), ())),
        precision=lax.Precision.DEFAULT,
        preferred_element_type=jnp.float32,
    )


def parts(values, count):
    terms = []
    for index in range(count):
        terms.append(values.astype(jnp.bfloat16))
        if index + 1 < count:
            values = values - terms[-1].astype(jnp.float32)
    return terms


def picked(values, choice):
    rows = values.shape[0]
    sums = dot(jnp.concatenate(parts(values, 3), axis=0), choice)
    return sums[:rows] + (sums[rows : 2 * rows] + sums[2 * rows :])


def table_dot(high, low, values):
    width = values.shape[1]
    large, small = parts(values, 2)
    sums = dot(high, jnp.concatenate([large, small], axis=1))
    return sums[:, :width] + (sums[:, width:] + dot(low, large))


def dot_table(values, high, low):
    rows = values.shape[0]
    large, small = parts(values, 2)
    sums = dot(jnp.concatenate([large, small], axis=0), high)
    return sums[:rows] + (sums[rows:] + dot(large, low))


def lanes_of(rows):
    return lax.broadcasted_iota(jnp.int32, (rows, LANES), 1)


def pack_for(out, dest, sides):
    lane = lanes_of(TILE_Z)
    packed = jnp.zeros((TILE_Z, LANES), jnp.float32)
    for index, values in enumerate(sides):
        moved = roll(values, index * SLOT - (4 * dest - 3), 1)
        here = (lane >= index * SLOT) & (lane < index * SLOT + 10)
        packed = jnp.where(here, moved, packed)
    own_lane = lanes_of(8) % SLOT < 10
    low = lax.broadcasted_iota(jnp.int32, (8, LANES), 0) < 4
    last = packed[8:]
    turned = roll(last, 4, 0)
    rest = jnp.where(low, roll(turned, 10, 1), roll(last, 6, 1))
    place = dest * SENT
    out[place : place + 8] = jnp.where(own_lane, packed[:8], rest)
    out[place + 8 : place + SENT] = jnp.where(own_lane, last, roll(turned, 2, 1))[:4]


def inner_body(*refs):
    far = refs[:9]
    out, flow, slope, mask_z, mask_x = refs[9:14]
    near = refs[14:23]
    downflow, shear, counts = refs[20:23]
    done = refs[23]
    fetches = [
        pltpu.make_async_copy(source, target, done.at[index])
        for index, (source, target) in enumerate(zip(far, near))
    ]
    for fetch in fetches:
        fetch.start()
    fetches[0].wait()
    cells = [near[0][c, p] for c in range(3) for p in range(PLANES)]
    for dest in range(1, GZ - 1):
        pack_for(out, dest, cells)
    for fetch in fetches[6:]:
        fetch.wait()
    lane = lanes_of(8)
    plane = lane % STRIDE // SLOT
    speeds = jnp.zeros((8, LANES), jnp.float32)
    shears = jnp.zeros((8, LANES), jnp.float32)
    for p in range(PLANES):
        speeds = jnp.where(plane == p, downflow[p], speeds)
        shears = jnp.where((plane == p) & (lane < STRIDE), shear[p], shears)
    flow[...] = speeds
    slope[...] = shears
    mode = lax.broadcasted_iota(jnp.int32, (MODES, LANES), 0)
    number = jnp.where(mode < HALF, mode, mode - HALF + 1)
    plane = lanes_of(MODES) % PLANES
    for mask, axis, length in ((mask_z, 1, NZ), (mask_x, 0, NX)):
        limit = jnp.zeros((MODES, LANES), jnp.int32)
        for p in range(PLANES):
            limit = jnp.where(plane == p, counts[axis, p], limit)
        weight = jnp.where(mode == 0, 1.0 / length, 2.0 / length)
        mask[...] = jnp.where(number <= limit, weight, 0.0)
    for fetch in fetches[1:6]:
        fetch.wait()


def outer_body(own, left, right, inner, out):
    low = lanes_of(TILE_Z) < LANES // 2
    pairs = [(c, p) for c in range(3) for p in range(PLANES)]
    pack_for(out, 0, [jnp.where(low, own[c, p], left[c, p]) for c, p in pairs])
    pack_for(out, GZ - 1, [jnp.where(low, right[c, p], own[c, p]) for c, p in pairs])


def advance_body(
    cells, flow_row, slope_row, mask, table, synth, sort_fields, sort_cells,
    out, start, first, second,
):
    chunk = 64
    edge = 8
    lane = lanes_of(chunk)
    component = lane // STRIDE
    flow = jnp.broadcast_to(flow_row[:1], (chunk, LANES))
    slope = jnp.broadcast_to(slope_row[:1], (chunk, LANES))

    def store(ref, row, values):
        ref[edge + row : edge + row + chunk] = values
        if row == 0:
            ref[edge + NZ : edge + NZ + edge] = values[:edge]
        if row == NZ - chunk:
            ref[:edge] = values[chunk - edge :]

    def rate(ref, row):
        low = edge + row
        middle = ref[low : low + chunk]
        north = ref[low + 1 : low + 1 + chunk]
        south = ref[low - 1 : low - 1 + chunk]
        east = roll(middle, -1, 1)
        west = roll(middle, 1, 1)
        next_one = roll(middle, -STRIDE, 1)
        along = jnp.where(
            component == 0,
            middle,
            jnp.where(component == 1, roll(middle, STRIDE, 1), roll(middle, 2 * STRIDE, 1)),
        )
        across = jnp.where(
            component == 2,
            middle,
            jnp.where(component == 1, next_one, roll(middle, -2 * STRIDE, 1)),
        )
        return middle, (
            -(flow + along) * ((east - west) * 0.5)
            - across * ((north - south) * 0.5)
            + molecular_diffusivity * (east + west + north + south - 4.0 * middle)
            - slope * next_one
        )

    rows = range(0, NZ, chunk)
    column = lanes_of(4) % SLOT
    for block in range(GZ):
        rest = jnp.zeros((4, LANES), jnp.float32)
        place = edge + block * 16
        for index in range(3):
            piece = cells[block * SENT + 4 * index : block * SENT + 4 * index + 4]
            start[place + 4 * index : place + 4 * index + 4] = piece
            rest = jnp.where(column // 4 == index, roll(piece, 4 * index - 10, 1), rest)
        start[place + SENT : place + 16] = rest
    start[:edge] = start[NZ : NZ + edge]
    start[edge + NZ :] = start[edge : 2 * edge]
    for row in rows:
        middle, change = rate(start, row)
        store(first, row, middle + time_step * change)
    for row in rows:
        middle, change = rate(first, row)
        begin = start[edge + row : edge + row + chunk]
        store(second, row, 0.75 * begin + 0.25 * (middle + time_step * change))
    part = (lane + LANES - 3) % LANES % SLOT // 4
    part = jnp.where((lane >= 3) & (lane < 127), part, 3)
    for row in rows:
        middle, change = rate(second, row)
        begin = start[edge + row : edge + row + chunk]
        last = begin * (1.0 / 3.0) + (2.0 / 3.0) * (middle + time_step * change)
        other = jnp.where(component == 2, roll(last, 2 * STRIDE, 1), roll(last, -STRIDE, 1))
        fields = jnp.where(part == 0, last, 0.0)
        fields = jnp.where(part == 1, roll(last * last, 4, 1), fields)
        first[row : row + chunk] = jnp.where(part == 2, roll(last * other, 8, 1), fields)
        sorted_cells = picked(jnp.where(part == 0, last, 0.0), sort_cells[...])
        start[edge + row : edge + row + chunk] = jnp.where(lane < 16, 0.0, sorted_cells)
        rest = jnp.where(lane < 16, sorted_cells, 0.0)
        rest = pltpu.roll(rest, 0, 1, stride=16, stride_axis=0)
        rest = jnp.sum(rest.reshape(chunk // 8, 8, LANES), axis=1)
        for block in range(chunk // 16):
            place = (row // 16 + block) * BACK + 16
            out[place : place + 2] = rest[2 * block : 2 * block + 2]
    coeffs = picked(table_dot(table[0], table[1], first[:NZ]), sort_fields[...]) * mask[...]
    filtered = table_dot(synth[0], synth[1], coeffs) + start[edge : edge + NZ]
    for block in range(GZ):
        out[block * BACK : block * BACK + 16] = filtered[16 * block : 16 * block + 16]


def forward_body(cells, out):
    for row in range(TILE_Z):
        out[row] = cells[pl.ds(row, GZ, stride=BACK), :]


def unsort():
    source = lax.broadcasted_iota(jnp.int32, (LANES, LANES), 0)
    target = lax.broadcasted_iota(jnp.int32, (LANES, LANES), 1)
    return jnp.where(target == source % 32 * 4 + source // 32, 1.0, 0.0).astype(jnp.bfloat16)


def cells_body(cells, out, rows):
    lane = lanes_of(8)
    rest = jnp.concatenate(
        [cells[pl.ds(16 + half, GZ, stride=BACK), :] for half in range(2)] * 2, axis=0
    ).T
    for group in range(4):
        turned = jnp.concatenate(
            [cells[pl.ds(4 * group + r, GZ, stride=BACK), :] for r in range(4)], axis=0
        ).T
        for r in range(4):
            row = 4 * group + r
            for begin, source, count, at in (
                (4 * FIELDS, turned, 5, r),
                (row % 8 * 16, rest, 4, row // 8),
            ):
                joined = jnp.zeros((count, LANES), jnp.float32)
                for column in range(4):
                    low = begin + column * count
                    moved = roll(source[low : low + count], (column - at) * 32, 1)
                    joined = jnp.where(lane[:count] // 32 == column, moved, joined)
                place = row * 16 + (0 if count == 5 else 5)
                rows[place : place + count] = joined
            rows[row * 16 + 9 : row * 16 + 16] = jnp.zeros((7, LANES), jnp.float32)
    order = unsort()
    rows[...] = picked(rows[...], order)
    for c in range(3):
        for p in range(PLANES):
            out[c, p] = rows[pl.ds(c * PLANES + p, TILE_Z, stride=16), :]


def streamwise_body(lines, mask, table, out, rows):
    cells = lines[...].reshape(NX // 4, LANES)
    coeffs = table_dot(table[0, 0], table[0, 1], cells)
    for column in range(1, 4):
        coeffs = coeffs + roll(
            table_dot(table[column, 0], table[column, 1], cells), -FIELDS * column, 1
        )
    coeffs = jnp.where(lanes_of(MODES) < FIELDS, coeffs * mask[...], 0.0).T[:32]
    rows[...] = jnp.zeros(rows.shape, jnp.float32)
    for column in range(4):
        filtered = dot_table(coeffs, table[column, 0], table[column, 1])
        for q, (a, b) in enumerate(zip(pair_first, pair_second)):
            rows[column, 3 * q : 3 * q + 3] = (
                filtered[9 + 3 * q : 12 + 3 * q]
                - filtered[3 * a : 3 * a + 3] * filtered[3 * b : 3 * b + 3]
            )
    lane = lanes_of(24)
    for dest in range(GX):
        begin = dest // 4 * LANES
        joined = jnp.zeros((24, LANES), jnp.float32)
        for column in range(4):
            moved = roll(rows[column, :, begin : begin + LANES], (column - dest % 4) * 32, 1)
            joined = jnp.where(lane // 32 == column, moved, joined)
        out[dest * STRESSES : (dest + 1) * STRESSES] = joined[:STRESSES]


def stress_body(lines, out, rows):
    rows[...] = picked(lines[...], unsort())
    for q in range(6):
        for p in range(PLANES):
            out[q, p] = rows[pl.ds(q * PLANES + p, TILE_Z, stride=STRESSES), :]


def wave_table(length):
    column = np.arange(MODES)
    numbers = np.where(column < HALF, column, column - HALF + 1)
    angles = (np.arange(length)[:, None] * numbers[None, :] % length) * (2.0 * math.pi / length)
    return np.where(column[None, :] < HALF, np.cos(angles), np.sin(angles))


def wave_tables():
    synth_z = wave_table(NZ).T
    synth_x = wave_table(NX).reshape(NX // 4, 4, MODES).transpose(1, 2, 0)
    sort_fields = np.zeros((LANES, LANES))
    sort_cells = np.zeros((LANES, LANES))
    kinds = ((0, 1, 2), (3, 6, 8), (4, 7, 5))
    for c in range(3):
        for p in range(PLANES):
            for column in range(4):
                lane = c * STRIDE + p * SLOT + 3 + column
                for kind in range(3):
                    field = kinds[kind][c] * PLANES + p
                    sort_fields[lane + 4 * kind, column * FIELDS + field] = 1.0
                index = c * PLANES + p
                if index < 5:
                    sort_cells[lane, 4 * FIELDS + column * 5 + index] = 1.0
                else:
                    sort_cells[lane, column * 4 + index - 5] = 1.0

    def halves(values):
        high = values.astype(jnp.bfloat16)
        low = (values - high.astype(np.float64)).astype(jnp.bfloat16)
        return np.stack([high, low], axis=-3)

    return [
        jnp.asarray(np.ascontiguousarray(values))
        for values in (
            halves(synth_z),
            halves(synth_z.T),
            sort_fields.astype(jnp.bfloat16),
            sort_cells.astype(jnp.bfloat16),
            halves(synth_x),
        )
    ]


def exchange(rows, axis, count):
    sent = rows.reshape(count, -1, 2, LANES)
    return lax.all_to_all(sent, axis, 0, 0, tiled=True).reshape(rows.shape)


def local(velocity, downflow, shear, mode_counts):
    count = lax.axis_size("gx")
    mode_counts = mode_counts.T
    left = lax.ppermute(velocity, "gx", [(i, (i + 1) % count) for i in range(count)])
    right = lax.ppermute(velocity, "gx", [((i + 1) % count, i) for i in range(count)])
    tables = [velocity, *wave_tables()]
    inner, flow, slope, mask_z, mask_x, *tables = call(
        inner_body,
        [(GZ * SENT, LANES), (8, LANES), (8, LANES), (MODES, LANES), (MODES, LANES), *tables],
        0,
        [],
        *tables,
        downflow,
        shear,
        mode_counts,
        tables=9,
        extra=[
            pltpu.SMEM((PLANES,), jnp.float32),
            pltpu.SMEM((PLANES,), jnp.float32),
            pltpu.SMEM((2, PLANES), jnp.int32),
        ],
    )
    own, analysis_z, synth_z, sort_fields, sort_cells, synth_x = tables
    (cells,) = call(
        outer_body,
        [(GZ * SENT, LANES)],
        0,
        [],
        own,
        left,
        right,
        inner,
        alias={3: 0},
    )
    cells = exchange(cells, spanwise, GZ)
    (cells,) = call(
        advance_body,
        [(GZ * BACK, LANES)],
        0,
        [(NZ + 16, LANES)] * 3,
        cells,
        flow,
        slope,
        mask_z,
        analysis_z,
        synth_z,
        sort_fields,
        sort_cells,
    )
    cells = exchange(cells, spanwise, GZ)
    (lines,) = call(forward_body, [(GX, GZ, LANES)], 0, [], cells)
    (advanced,) = call(
        cells_body, [(3, PLANES, TILE_Z, TILE_X)], 0, [(16 * TILE_Z, LANES)], cells, final=True
    )
    lines, advanced = lax.optimization_barrier((lines, advanced))
    lines = lax.all_to_all(lines, "gx", 0, 0, tiled=True)
    (lines,) = call(
        streamwise_body,
        [(GX * STRESSES, LANES)],
        0,
        [(4, 24, NX // 4)],
        lines,
        mask_x,
        synth_x,
    )
    lines = exchange(lines, "gx", GX)
    (stress,) = call(
        stress_body, [(6, PLANES, TILE_Z, TILE_X)], 0, [(GX * STRESSES, LANES)], lines, final=True
    )
    return advanced, stress


def solution(mesh):
    return jax.shard_map(
        local,
        mesh=mesh,
        in_specs=(P(None, None, ("gz", "grp"), "gx"), P(), P(), P()),
        out_specs=(P(None, None, ("gz", "grp"), "gx"), P(None, None, ("gz", "grp"), "gx")),
        check_vma=False,
    )
```
